32 devices in a mesh: occ: 4 (over x, core), vir: 8 (over z, y).
Axes of the slice: x: 2, y: 2, z: 4, core: 2. Of those that a mesh axis runs over, the one named last changes fastest.
Arguments:
- factor: float32 [4, 4096, 1280], P('occ', 'vir'), may hold values from -0.6 to 0.6
- occ_energy: float32 [4], P('occ'), may hold values from -2 to -0.5
- vir_energy: float32 [4096], P('vir'), may hold values from 0.2 to 4.7
Outputs:
- aux_density: float32 [4, 4096, 1280], P('occ', 'vir')
- pair_trace: float32 [4, 3], P('occ')
The draws below stay inside these ranges and needn't reach their ends.
All inputs are finite; a program needn't handle non-finite values.
Results may differ from the reference program's by a relative error of at most 0.00013.
Values sent between devices are 32-bit elements; how exact they have to be, the bound alone decides.
No kernel may reach another device: no remote copies, remote signals or barrier semaphores. Data moves between devices by JAX's collectives and lax.ppermute only.
A program may use at most 128 MiB of HBM per device.

```python
import math
import jax
import jax.numpy as jnp
from jax import lax

NVIR = 4096
NAUX = 1280
OCC_DEV = 1
STEPS = 3
NOCC = 4
N_OCC = 4
N_VIR = 8


def draw_vir_energy(key, part):
    position = jnp.arange(NVIR, dtype=jnp.float32) / NVIR
    spread = jnp.exp(jax.random.uniform(key, (NVIR,), jnp.float32, math.log(0.7), math.log(1.4)))
    return (0.3 + 3.0 * position) * spread


def shard_levels(stream_key, extent, split, smallest, top_value):
    level, own = 1.0, jax.random.fold_in(stream_key, 6)
    for axis_at, shards_of in split:
        heights = jnp.exp(jax.random.uniform(jax.random.fold_in(own, axis_at), (shards_of,), jnp.float32, smallest / len(split), top_value / len(split)))
        level = level * jnp.repeat(heights, extent[axis_at] // shards_of).reshape([-1 if axis == axis_at else 1 for axis in range(len(extent))])
    return level


def bell_draw(key, shape, width, reach, split=(), kind=jnp.bfloat16):
    entries = jax.random.normal(key, shape, jnp.float32) * width
    if len(split) > 0:
        entries = shard_levels(key, shape, split, -0.22, 0.18) * entries
    return jnp.clip(entries, min=-reach, max=reach).astype(kind)


def setup_inputs(seed: int = 0) -> dict:
    key_list = jax.random.split(jax.random.key(seed), 4)
    factor = bell_draw(key_list[0], (NOCC, NVIR, NAUX), 0.09, 0.6, ((0, 4), (1, 8)), jnp.float32)
    occ_energy = jnp.clip(-2.0 + 1.5 * jax.random.uniform(key_list[1], (NOCC,), jnp.float32) ** shard_levels(key_list[1], (NOCC,), ((0, 4),), -0.2, 0.2), -2.0, -0.5)
    vir_energy = draw_vir_energy(jax.random.fold_in(key_list[3], 71), 0)
    return {"factor": factor, "occ_energy": occ_energy, "vir_energy": vir_energy}


def contract(pattern, former, latter):
    return jnp.einsum(pattern, former, latter, precision=lax.Precision.HIGHEST, preferred_element_type=jnp.float32)


def flip_pairs(tensor, dim_index):
    old_shape = tensor.shape
    new_shape = old_shape[:dim_index] + (old_shape[dim_index] // 2, 2) + old_shape[dim_index + 1:]
    return jnp.flip(tensor.reshape(new_shape), dim_index + 1).reshape(old_shape)


def reference(factor, occ_energy, vir_energy):
    vir_dev = NVIR // N_VIR
    occ_blocks = factor.reshape(N_OCC, OCC_DEV, N_VIR, vir_dev, NAUX)
    occ_levels = occ_energy.reshape(N_OCC, OCC_DEV)
    vir_levels = vir_energy.reshape(N_VIR, vir_dev)
    vir_far = flip_pairs(vir_levels, 0)
    density = jnp.zeros(occ_blocks.shape, jnp.float32)
    traces = []
    for offset in range(STEPS):
        cycle_rows = jnp.roll(occ_blocks, offset, axis=0)
        cycle_occ = jnp.roll(occ_levels, offset, axis=0)
        far_rows = flip_pairs(cycle_rows, 2)
        pair_occ = occ_levels[:, :, None] + cycle_occ[:, None, :]
        gap_diag = pair_occ[:, :, :, None, None, None] - vir_levels[None, None, None, :, :, None] - vir_levels[None, None, None, :, None, :]
        gap_off = pair_occ[:, :, :, None, None, None] - vir_levels[None, None, None, :, :, None] - vir_far[None, None, None, :, None, :]
        k_diag = contract("oivap,ojvbp->oijvab", occ_blocks, cycle_rows)
        k_off = contract("oivap,ojvbp->oijvab", occ_blocks, far_rows)
        amp_diag = k_diag / gap_diag
        amp_off = k_off / gap_off
        bar_diag = 2.0 * amp_diag - jnp.swapaxes(amp_diag, 4, 5)
        k_cross = jnp.swapaxes(flip_pairs(k_off, 3), 4, 5)
        bar_off = 2.0 * amp_off - k_cross / gap_off
        traces.append(jnp.sum(amp_diag * bar_diag + amp_off * bar_off, axis=(3, 4, 5)) / NVIR)
        density = density + contract("oijvab,ojvbp->oivap", bar_diag, cycle_rows) + contract("oijvab,ojvbp->oivap", bar_off, far_rows)
        returned = contract("oijvab,oivap->ojvbp", bar_diag, occ_blocks) + flip_pairs(contract("oijvab,oivap->ojvbp", bar_off, occ_blocks), 2)
        density = density + jnp.roll(returned, -offset, axis=0)
    pair_trace = jnp.stack(traces, axis=2).reshape(N_OCC * OCC_DEV, STEPS * OCC_DEV)
    return density.reshape(N_OCC * OCC_DEV, NVIR, NAUX), pair_trace
```

```python
import jax
import jax.numpy as jnp
from jax import lax
from jax.sharding import PartitionSpec as P

STEPS = 3
AXES = ("occ", "vir")


def permuted(value, move):
    occs, virs = lax.axis_size("occ"), lax.axis_size("vir")
    route = []
    for i in range(occs):
        for v in range(virs):
            source = move(i, v)
            route.append((source[0] % occs * virs + source[1], i * virs + v))
    return lax.ppermute(value, AXES, route)


def contract(pattern, former, latter):
    return jnp.einsum(
        pattern, former, latter, precision=lax.Precision.HIGH, preferred_element_type=jnp.float32
    )


def weight(offset, occs):
    return sum(offset == k % occs for k in range(STEPS)) + sum(
        offset == -k % occs for k in range(STEPS)
    )


def local(factor, occ_energy, vir_energy):
    occs = lax.axis_size("occ")
    rows = factor.shape[1]
    nvir = rows * lax.axis_size("vir")
    own = factor[0]
    half = rows // 2
    me = lax.axis_index("occ")
    far_vir = permuted(vir_energy, lambda i, v: (i, v ^ 1))

    if occs == 4:
        moves = [1, 2, 3]
        occ_of = {m: permuted(occ_energy, lambda i, v, m=m: (i ^ m, v)) for m in moves}
        near, far = {0: own}, {}
        near[1] = permuted(own, lambda i, v: (i ^ 1, v))
        near[2] = permuted(own, lambda i, v: (i ^ 2, v))
        far[0] = permuted(own, lambda i, v: (i, v ^ 1))
        near[3] = permuted(near[2], lambda i, v: (i ^ 1, v))
        far[1] = permuted(far[0], lambda i, v: (i ^ 1, v))
        low = permuted(far[0][:half], lambda i, v: (i ^ 2, v))
        high = permuted(near[2][half:], lambda i, v: (i, v ^ 1))
        far[2] = jnp.concatenate([low, high], axis=0)
        far[3] = permuted(far[2], lambda i, v: (i ^ 1, v))
        weights = {1: weight(1, occs), 2: weight(2, occs), 3: weight(1, occs)}
    else:
        moves = [d for d in range(1, occs) if weight(d, occs) > 0]
        occ_of = {d: permuted(occ_energy, lambda i, v, d=d: (i - d, v)) for d in moves}
        near, far = {0: own}, {0: permuted(own, lambda i, v: (i, v ^ 1))}
        for d in moves:
            near[d] = permuted(own, lambda i, v, d=d: (i - d, v))
            far[d] = permuted(near[d], lambda i, v: (i, v ^ 1))
        weights = {d: weight(d, occs) for d in moves}

    sums_near = -vir_energy[:, None] - vir_energy[None, :]
    sums_far = -vir_energy[:, None] - far_vir[None, :]
    trace_of = {}

    pair_occ = occ_energy[0] + occ_energy[0]
    t_near = contract("ap,bp->ab", own, own) / (pair_occ + sums_near)
    t_far = contract("ap,bp->ab", own, far[0]) / (pair_occ + sums_far)
    trace_of[0] = jnp.sum(t_near * t_near) + jnp.sum(t_far * t_far)
    w0 = weight(0, occs)
    density = w0 * (contract("ab,bp->ap", t_near, own) + contract("ab,bp->ap", t_far, far[0]))
    for m in moves:
        pair_occ = occ_energy[0] + occ_of[m][0]
        t_near = contract("ap,bp->ab", own, near[m]) / (pair_occ + sums_near)
        bar_near = 2.0 * t_near - t_near.T
        density = density + weights[m] * contract("ab,bp->ap", bar_near, near[m])
        gap_far = pair_occ + sums_far
        t_far = contract("ap,bp->ab", own, far[m]) / gap_far
        t_cross = contract("ap,bp->ab", near[m], far[0]) / gap_far
        bar_far = 2.0 * t_far - t_cross
        density = density + weights[m] * contract("ab,bp->ap", bar_far, far[m])
        trace_of[m] = jnp.sum(t_near * bar_near) + jnp.sum(t_far * bar_far)

    traces = []
    for k in range(STEPS):
        if occs == 4 and k % 2 == 1:
            traces.append(jnp.where((me ^ (me - k) % occs) == 1, trace_of[1], trace_of[3]))
        else:
            traces.append(trace_of[k % occs])
    pair_trace = lax.psum(jnp.stack(traces)[None] / nvir, "vir")
    return density[None], pair_trace


def solution(mesh):
    placed = (P("occ", "vir", None), P("occ"), P("vir"))
    return jax.shard_map(
        local,
        mesh=mesh,
        in_specs=placed,
        out_specs=(P("occ", "vir", None), P("occ", None)),
        check_vma=False,
    )
```

```python
import functools

import jax
import jax.numpy as jnp
from jax import lax
from jax.experimental import pallas as pl
from jax.experimental.pallas import tpu as pltpu
from jax.sharding import PartitionSpec as P

STEPS = 3
AXES = ("occ", "vir")
F32, BF16 = jnp.float32, jnp.bfloat16


def permuted(value, move):
    occs, virs = lax.axis_size("occ"), lax.axis_size("vir")
    route = []
    for i in range(occs):
        for v in range(virs):
            source = move(i, v)
            route.append((source[0] % occs * virs + source[1], i * virs + v))
    return lax.ppermute(value, AXES, route)


def weight(offset, occs):
    return sum(offset == k % occs for k in range(STEPS)) + sum(
        offset == -k % occs for k in range(STEPS)
    )


def split(value):
    high = value.astype(BF16)
    return high, (value - high.astype(F32)).astype(BF16)


def dot(former, latter, transposed):
    contracted = ((1,), (1 if transposed else 0,))
    return lax.dot_general(
        former, latter, (contracted, ((), ())), preferred_element_type=F32
    )


def product(former, latter, transposed):
    (fh, fl), (lh, ll) = former, latter
    return dot(fh, lh, transposed) + dot(fh, ll, transposed) + dot(fl, lh, transposed)


def column(row):
    return jnp.transpose(jnp.broadcast_to(row, (8, row.shape[1])))[:, :1]


def lanes(value):
    return jnp.sum(value, axis=0, keepdims=True)


def load(source, target, sem):
    copy = pltpu.make_async_copy(source, target, sem)
    copy.start()
    return copy


def load_either(odd, for_even, for_odd, target, sem):
    @pl.when(odd == 0)
    def _():
        pltpu.make_async_copy(for_even, target, sem).start()

    @pl.when(odd == 1)
    def _():
        pltpu.make_async_copy(for_odd, target, sem).start()

    return pltpu.make_async_copy(for_even, target, sem)


def is_odd():
    return lax.rem(lax.axis_index("occ"), 2)


def own_kernel(occ, vir, rows, high, low, total, trace, bar_h, bar_l):
    high[...], low[...] = split(rows[...])
    own = (high[...], low[...])
    gap = occ[0] - column(vir[...]) - vir[...]
    amp = product(own, own, True) / gap
    trace[...] = lanes(amp * amp)
    bar_h[...], bar_l[...] = split(occ[8] * amp)
    total[...] = product((bar_h[...], bar_l[...]), own, False)


def near_kernel(pair, chosen, occ, vir, high, low, even_rows, odd_rows, before, total, trace,
                rows, rows_h, rows_l, held, bar_h, bar_l, sems):
    if chosen:
        rows_copy = load_either(is_odd(), even_rows, odd_rows, rows, sems.at[0])
    else:
        rows_copy = load(even_rows, rows, sems.at[0])
    held_copy = load(before, held, sems.at[1])
    rows_copy.wait()
    rows_h[...], rows_l[...] = split(rows[...])
    halves = (rows_h[...], rows_l[...])
    gap = occ[pair] - column(vir[...]) - vir[...]
    amp = product((high[...], low[...]), halves, True) / gap
    bar = 2.0 * amp - amp.T
    trace[...] = lanes(amp * bar)
    bar_h[...], bar_l[...] = split(occ[pair + 8] * bar)
    held_copy.wait()
    total[...] = held[...] + product((bar_h[...], bar_l[...]), halves, False)


def first_far_kernel(occ, vir, far, high, low, even_rows, odd_rows, before, total, amp_out,
                     rows, rows_h, rows_l, held, bar_h, bar_l, sems):
    rows_copy = load_either(is_odd(), even_rows, odd_rows, rows, sems.at[0])
    held_copy = load(before, held, sems.at[1])
    rows_copy.wait()
    rows_h[...], rows_l[...] = split(rows[...])
    halves = (rows_h[...], rows_l[...])
    gap = occ[6] - column(vir[...]) - far[...]
    amp = product((high[...], low[...]), halves, True) / gap
    amp_out[...] = amp
    bar_h[...], bar_l[...] = split(occ[14] * amp)
    held_copy.wait()
    total[...] = held[...] + product((bar_h[...], bar_l[...]), halves, False)


def second_far_kernel(occ, vir, far, high, low, near_rows, first, second_even, second_odd,
                      amp_first, before, total, trace_own, trace_near, far_h, far_l,
                      rows, near_h, near_l, rows_h, rows_l, amps, held, bar_h, bar_l, sems):
    odd = is_odd()
    slot = odd
    near_copy = load(near_rows, rows.at[2], sems.at[0])
    first_even, first_odd = first
    one = load_either(odd, first_even, first_odd, rows.at[1 - slot], sems.at[1])
    two = load_either(odd, second_even, second_odd, rows.at[slot], sems.at[2])
    amp_copy = load(amp_first, amps.at[1 - slot], sems.at[3])
    held_copy = load(before, held, sems.at[4])
    one.wait()
    two.wait()
    for s in range(2):
        rows_h[s], rows_l[s] = split(rows[s])
    far_h[...], far_l[...] = rows_h[0], rows_l[0]
    near_copy.wait()
    near_h[...], near_l[...] = split(rows[2])
    sums = column(vir[...]) + far[...]
    halves = (rows_h[slot], rows_l[slot])
    amp = product((high[...], low[...]), halves, True) / (occ[7] - sums)
    amps[slot] = amp
    bar_h[...], bar_l[...] = split(occ[15] * amp)
    held_copy.wait()
    held[...] += product((bar_h[...], bar_l[...]), halves, False)
    cross = product((near_h[...], near_l[...]), (rows_h[0], rows_l[0]), True) / (occ[1] - sums)
    bar_h[...], bar_l[...] = split(-occ[9] * cross)
    amp_copy.wait()
    own_amp, near_amp = amps[0], amps[1]
    trace_own[...] = lanes(own_amp * own_amp)
    trace_near[...] = lanes(near_amp * (2.0 * near_amp - cross))
    total[...] = held[...] + product((bar_h[...], bar_l[...]), (rows_h[1], rows_l[1]), False)


def near_cross_kernel(occ, vir, far, high, low, far_h, far_l, first, second, before,
                      total, trace, crosses,
                      rows, rows_h, rows_l, held, bar_h, bar_l, sems):
    odd = is_odd()
    two = load_either(odd, second[0], second[1], rows.at[1], sems.at[1])
    one = load_either(odd, first[0], first[1], rows.at[0], sems.at[0])
    held_copy = load(before, held, sems.at[2])
    two.wait()
    rows_h[...], rows_l[...] = split(rows[1])
    halves = (rows_h[...], rows_l[...])
    col = column(vir[...])
    amp = product((high[...], low[...]), halves, True) / (occ[3] - col - vir[...])
    bar = 2.0 * amp - amp.T
    trace[...] = lanes(amp * bar)
    bar_h[...], bar_l[...] = split(occ[11] * bar)
    held_copy.wait()
    total[...] = held[...] + product((bar_h[...], bar_l[...]), halves, False)
    other = (far_h[...], far_l[...])
    crosses[1 - odd] = product(halves, other, True) / (occ[3] - col - far[...])
    one.wait()
    rows_h[...], rows_l[...] = split(rows[0])
    halves = (rows_h[...], rows_l[...])
    crosses[odd] = product(halves, other, True) / (occ[2] - col - far[...])


def last_far_kernel(pair, which, start, occ, vir, far, high, low, far_rows, crosses, before,
                    total, trace, rows, rows_h, rows_l, cross, held, bar_h, bar_l, sems):
    size = rows.shape[0]
    rows_copy = load(far_rows, rows, sems.at[0])
    held_copy = load(before, held, sems.at[1])
    cross_copy = load(crosses.at[which], cross, sems.at[2])
    rows_copy.wait()
    rows_h[...], rows_l[...] = split(rows[...])
    halves = (rows_h[...], rows_l[...])
    part = slice(start, start + size)
    gap = occ[pair] - column(vir[...]) - far[:, part]
    amp = product((high[...], low[...]), halves, True) / gap
    cross_copy.wait()
    bar = 2.0 * amp - cross[:, part]
    trace[...] = lanes(amp * bar)
    bar_h[...], bar_l[...] = split(occ[pair + 8] * bar)
    held_copy.wait()
    total[...] = held[...] + product((bar_h[...], bar_l[...]), halves, False)


VMEM = pl.BlockSpec(memory_space=pltpu.VMEM)
SMEM = pl.BlockSpec(memory_space=pltpu.SMEM)
HBM = pl.BlockSpec(memory_space=pltpu.HBM)


def call(kernel, name, units, inputs, outputs, scratch, aliases=None):
    leaves, tree = jax.tree.flatten(inputs, is_leaf=lambda x: isinstance(x, tuple) and len(x) == 2 and isinstance(x[0], pl.BlockSpec))
    specs = [leaf[0] for leaf in leaves]
    arrays = [leaf[1] for leaf in leaves]
    count = len(arrays)

    def body(*refs):
        ins = jax.tree.unflatten(tree, refs[:count])
        kernel(*ins, *refs[count:])

    return pl.pallas_call(
        body,
        name=name,
        in_specs=specs,
        out_specs=tuple(o[0] for o in outputs),
        out_shape=tuple(jax.ShapeDtypeStruct(o[1], o[2]) for o in outputs),
        scratch_shapes=scratch,
        input_output_aliases=aliases or {},
        compiler_params=pltpu.CompilerParams(vmem_limit_bytes=40 * 2**20),
        cost_estimate=pl.CostEstimate(
            flops=int(units * 2 * 3 * 512 * 512 * 1280), bytes_accessed=8 << 20, transcendentals=0
        ),
    )(*arrays)


def gathered_plane(factor, occ_energy, vir_energy):
    own = factor[0]
    rows, aux = own.shape
    half = rows // 2
    occs = lax.axis_size("occ")
    me = lax.axis_index("occ")
    odd = me % 2

    def core(value):
        return permuted(value, lambda i, v: (i ^ 1, v))

    def mixed(value, parity):
        return permuted(value, lambda i, v: (i ^ 2, v) if i % 2 == parity else (i, v ^ 1))

    far_vir = permuted(vir_energy, lambda i, v: (i, v ^ 1))
    e = {0: occ_energy[0]}
    for m in (1, 2, 3):
        e[m] = permuted(occ_energy, lambda i, v, m=m: (i ^ m, v))[0]
    near = core(own)
    first = mixed(own, 0)
    own_again, first = lax.optimization_barrier((own, first))
    second = mixed(own_again, 1)
    first_core = core(first)
    low_part = mixed(first[:half], 1)
    high_part = mixed(first[half:], 1)
    second_core = core(second)
    low_core, high_core = core(low_part), core(high_part)

    w0, w1, w2 = weight(0, occs), weight(1, occs), weight(2, occs)
    e1 = jnp.where(odd == 0, e[2], e[3])
    e2 = jnp.where(odd == 0, e[3], e[2])
    wn1 = jnp.where(odd == 0, w2, w1).astype(F32)
    wn2 = jnp.where(odd == 0, w1, w2).astype(F32)
    ef1 = jnp.where(odd == 0, e[1], e[0])
    ef2 = jnp.where(odd == 0, e[0], e[1])
    wf1 = jnp.where(odd == 0, 2 * w1, w0).astype(F32)
    wf2 = jnp.where(odd == 0, w0, 2 * w1).astype(F32)
    pairs = [e[0], e[1], e1, e2, e[2], e[3], ef1, ef2]
    weights = [jnp.asarray(w, F32) for w in (w0, w1, wn1, wn2, w2, w1, wf1, wf2)]
    occ = jnp.stack([e[0] + p for p in pairs] + weights)
    vir, far = vir_energy[None, :], far_vir[None, :]

    block = (rows, aux)
    square = (rows, rows)
    full = pltpu.VMEM(block, F32)
    full_h = pltpu.VMEM(block, BF16)
    bar = pltpu.VMEM(square, BF16)
    sems = pltpu.SemaphoreType.DMA((5,))
    line = (VMEM, (1, rows), F32)
    total_out = (HBM, block, F32)
    dense = (VMEM, block, F32)

    high, low, density, trace_own = call(
        own_kernel, "own", 2,
        [(SMEM, occ), (VMEM, vir), (VMEM, own)],
        [(VMEM, block, BF16), (VMEM, block, BF16), dense, line],
        [bar, bar],
    )
    scratch = [full, full_h, full_h, full, bar, bar, sems]
    density, trace_1n = call(
        functools.partial(near_kernel, 1, False), "near", 2,
        [(SMEM, occ), (VMEM, vir), (VMEM, high), (VMEM, low), (HBM, near), (HBM, near), (HBM, density)],
        [dense, line], scratch,
    )
    density, trace_n1 = call(
        functools.partial(near_kernel, 2, True), "near", 2,
        [(SMEM, occ), (VMEM, vir), (VMEM, high), (VMEM, low), (HBM, first), (HBM, first_core), (HBM, density)],
        [dense, line], scratch,
    )
    density, amp_first = call(
        first_far_kernel, "first_far", 2,
        [(SMEM, occ), (VMEM, vir), (VMEM, far), (VMEM, high), (VMEM, low), (HBM, first_core), (HBM, first), (HBM, density)],
        [dense, (VMEM, square, F32)], scratch,
    )
    density, trace_0f, trace_1f, far_h, far_l = call(
        second_far_kernel, "second_far", 4,
        [(SMEM, occ), (VMEM, vir), (VMEM, far), (VMEM, high), (VMEM, low), (HBM, near),
         [(HBM, first_core), (HBM, first)], (HBM, second), (HBM, second_core), (HBM, amp_first), (HBM, density)],
        [dense, line, line, (VMEM, block, BF16), (VMEM, block, BF16)],
        [pltpu.VMEM((3, *block), F32), full_h, full_h, pltpu.VMEM((2, *block), BF16), pltpu.VMEM((2, *block), BF16),
         pltpu.VMEM((2, *square), F32), full, bar, bar, sems],
    )
    density, trace_n2, crosses = call(
        near_cross_kernel, "near_cross", 4,
        [(SMEM, occ), (VMEM, vir), (VMEM, far), (VMEM, high), (VMEM, low), (VMEM, far_h), (VMEM, far_l),
         [(HBM, first), (HBM, first_core)], [(HBM, second_core), (HBM, second)], (HBM, density)],
        [dense, line, (VMEM, (2, *square), F32)],
        [pltpu.VMEM((2, *block), F32), full_h, full_h, full, bar, bar, sems],
    )

    part = (half, aux)
    part_bar = pltpu.VMEM((rows, half), BF16)
    scratch = [pltpu.VMEM(part, F32), pltpu.VMEM(part, BF16), pltpu.VMEM(part, BF16),
               pltpu.VMEM(square, F32), full, part_bar, part_bar, sems]
    last = {2: [], 3: []}
    for start, parts in ((0, (low_part, low_core)), (half, (high_part, high_core))):
        for which, (move, value) in enumerate(zip((2, 3), parts)):
            density, trace = call(
                functools.partial(last_far_kernel, 2 + move, which, start), "last_far", 1,
                [(SMEM, occ), (VMEM, vir), (VMEM, far), (VMEM, high), (VMEM, low), (HBM, value), (HBM, crosses), (HBM, density)],
                [dense, (VMEM, (1, half), F32)], scratch,
            )
            last[move].append(trace)

    trace_near = {0: jnp.sum(trace_own + trace_0f), 1: jnp.sum(trace_1n + trace_1f)}
    sum_n1, sum_n2 = jnp.sum(trace_n1), jnp.sum(trace_n2)
    trace_near[2] = jnp.where(odd == 0, sum_n1, sum_n2) + jnp.sum(last[2][0] + last[2][1])
    trace_near[3] = jnp.where(odd == 0, sum_n2, sum_n1) + jnp.sum(last[3][0] + last[3][1])
    traces = [trace_near[0], jnp.where(odd == 1, trace_near[1], trace_near[3]), trace_near[2]]
    return density[None], jnp.stack(traces)


def contract(pattern, former, latter):
    return jnp.einsum(
        pattern, former, latter, precision=lax.Precision.HIGH, preferred_element_type=F32
    )


def gathered_ring(factor, occ_energy, vir_energy):
    own = factor[0]
    occs = lax.axis_size("occ")
    far_vir = permuted(vir_energy, lambda i, v: (i, v ^ 1))
    own_far = permuted(own, lambda i, v: (i, v ^ 1))
    sums_near = vir_energy[:, None] + vir_energy[None, :]
    sums_far = vir_energy[:, None] + far_vir[None, :]
    density, trace_of = 0.0, {}
    for d in range(occs):
        if weight(d, occs) == 0:
            continue
        near = permuted(own, lambda i, v, d=d: (i - d, v))
        far = permuted(near, lambda i, v: (i, v ^ 1))
        pair = occ_energy[0] + permuted(occ_energy, lambda i, v, d=d: (i - d, v))[0]
        amp_near = contract("ap,bp->ab", own, near) / (pair - sums_near)
        amp_far = contract("ap,bp->ab", own, far) / (pair - sums_far)
        cross = contract("ap,bp->ab", near, own_far) / (pair - sums_far)
        bar_near = 2.0 * amp_near - amp_near.T
        bar_far = 2.0 * amp_far - cross
        density = density + weight(d, occs) * (
            contract("ab,bp->ap", bar_near, near) + contract("ab,bp->ap", bar_far, far)
        )
        trace_of[d] = jnp.sum(amp_near * bar_near) + jnp.sum(amp_far * bar_far)
    return density[None], jnp.stack([trace_of[k % occs] for k in range(STEPS)])


def local(factor, occ_energy, vir_energy):
    gathered = gathered_plane if lax.axis_size("occ") == 4 else gathered_ring
    density, traces = gathered(factor, occ_energy, vir_energy)
    nvir = factor.shape[1] * lax.axis_size("vir")
    return density, lax.psum(traces[None] / nvir, "vir")


def solution(mesh):
    placed = (P("occ", "vir", None), P("occ"), P("vir"))
    return jax.shard_map(
        local,
        mesh=mesh,
        in_specs=placed,
        out_specs=(P("occ", "vir", None), P("occ", None)),
        check_vma=False,
    )
```

```python
import functools

import jax
import jax.numpy as jnp
from jax import lax
from jax.experimental import pallas as pl
from jax.experimental.pallas import tpu as pltpu
from jax.sharding import PartitionSpec as P


STEPS = 3
AXES = ("occ", "vir")
F32, BF16 = jnp.float32, jnp.bfloat16


def permuted(value, move):
    occs, virs = lax.axis_size("occ"), lax.axis_size("vir")
    route = []
    for i in range(occs):
        for v in range(virs):
            source = move(i, v)
            route.append((source[0] % occs * virs + source[1], i * virs + v))
    return lax.ppermute(value, AXES, route)


def weight(offset, occs):
    return sum(offset == k % occs for k in range(STEPS)) + sum(
        offset == -k % occs for k in range(STEPS)
    )


def split(value):
    high = value.astype(BF16)
    return high, (value - high.astype(F32)).astype(BF16)


def dot(former, latter, transposed):
    contracted = ((1,), (1 if transposed else 0,))
    return lax.dot_general(
        former, latter, (contracted, ((), ())), preferred_element_type=F32
    )


def product(former, latter, transposed):
    (fh, fl), (lh, ll) = former, latter
    return dot(fh, lh, transposed) + dot(fh, ll, transposed) + dot(fl, lh, transposed)


def column(row):
    return jnp.transpose(jnp.broadcast_to(row, (8, row.shape[1])))[:, :1]


def lanes(value):
    return jnp.sum(value, axis=0, keepdims=True)


def load(source, target, sem):
    copy = pltpu.make_async_copy(source, target, sem)
    copy.start()
    return copy


def load_either(odd, for_even, for_odd, target, sem):
    @pl.when(odd == 0)
    def _():
        pltpu.make_async_copy(for_even, target, sem).start()

    @pl.when(odd == 1)
    def _():
        pltpu.make_async_copy(for_odd, target, sem).start()

    return pltpu.make_async_copy(for_even, target, sem)


def is_odd():
    return lax.rem(lax.axis_index("occ"), 2)


def own_kernel(occ, vir, rows, high, low, total, trace, bar_h, bar_l):
    high[...], low[...] = split(rows[...])
    own = (high[...], low[...])
    gap = occ[0] - column(vir[...]) - vir[...]
    amp = product(own, own, True) / gap
    trace[...] = lanes(amp * amp)
    bar_h[...], bar_l[...] = split(occ[8] * amp)
    total[...] = product((bar_h[...], bar_l[...]), own, False)


def near_kernel(pair, chosen, occ, vir, high, low, even_rows, odd_rows, before, total, trace,
                rows, rows_h, rows_l, bar_h, bar_l, sems):
    if chosen:
        rows_copy = load_either(is_odd(), even_rows, odd_rows, rows, sems.at[0])
    else:
        rows_copy = load(even_rows, rows, sems.at[0])
    rows_copy.wait()
    rows_h[...], rows_l[...] = split(rows[...])
    halves = (rows_h[...], rows_l[...])
    gap = occ[pair] - column(vir[...]) - vir[...]
    amp = product((high[...], low[...]), halves, True) / gap
    bar = 2.0 * amp - amp.T
    trace[...] = lanes(amp * bar)
    bar_h[...], bar_l[...] = split(occ[pair + 8] * bar)
    total[...] = before[...] + product((bar_h[...], bar_l[...]), halves, False)


def first_far_kernel(occ, vir, far, high, low, even_rows, odd_rows, before, total, amp_out,
                     rows, rows_h, rows_l, bar_h, bar_l, sems):
    rows_copy = load_either(is_odd(), even_rows, odd_rows, rows, sems.at[0])
    rows_copy.wait()
    rows_h[...], rows_l[...] = split(rows[...])
    halves = (rows_h[...], rows_l[...])
    gap = occ[6] - column(vir[...]) - far[...]
    amp = product((high[...], low[...]), halves, True) / gap
    amp_out[...] = amp
    bar_h[...], bar_l[...] = split(occ[14] * amp)
    total[...] = before[...] + product((bar_h[...], bar_l[...]), halves, False)


def second_far_kernel(occ, vir, far, high, low, near_rows, first, second_even, second_odd,
                      amp_first, before, total, trace_own, trace_near, far_h, far_l,
                      rows, near_h, near_l, rows_h, rows_l, amps, bar_h, bar_l, sems):
    odd = is_odd()
    slot = odd
    near_copy = load(near_rows, rows.at[2], sems.at[0])
    first_even, first_odd = first
    one = load_either(odd, first_even, first_odd, rows.at[1 - slot], sems.at[1])
    two = load_either(odd, second_even, second_odd, rows.at[slot], sems.at[2])
    amps[1 - slot] = amp_first[...]
    one.wait()
    two.wait()
    for s in range(2):
        rows_h[s], rows_l[s] = split(rows[s])
    far_h[...], far_l[...] = rows_h[0], rows_l[0]
    near_copy.wait()
    near_h[...], near_l[...] = split(rows[2])
    sums = column(vir[...]) + far[...]
    halves = (rows_h[slot], rows_l[slot])
    amp = product((high[...], low[...]), halves, True) / (occ[7] - sums)
    amps[slot] = amp
    bar_h[...], bar_l[...] = split(occ[15] * amp)
    total[...] = before[...] + product((bar_h[...], bar_l[...]), halves, False)
    cross = product((near_h[...], near_l[...]), (rows_h[0], rows_l[0]), True) / (occ[1] - sums)
    bar_h[...], bar_l[...] = split(-occ[9] * cross)
    own_amp, near_amp = amps[0], amps[1]
    trace_own[...] = lanes(own_amp * own_amp)
    trace_near[...] = lanes(near_amp * (2.0 * near_amp - cross))
    total[...] += product((bar_h[...], bar_l[...]), (rows_h[1], rows_l[1]), False)


def near_cross_kernel(occ, vir, far, high, low, far_h, far_l, first, second, before,
                      total, trace, crosses,
                      rows, rows_h, rows_l, bar_h, bar_l, sems):
    odd = is_odd()
    two = load_either(odd, second[0], second[1], rows.at[1], sems.at[1])
    one = load_either(odd, first[0], first[1], rows.at[0], sems.at[0])
    two.wait()
    rows_h[...], rows_l[...] = split(rows[1])
    halves = (rows_h[...], rows_l[...])
    col = column(vir[...])
    amp = product((high[...], low[...]), halves, True) / (occ[3] - col - vir[...])
    bar = 2.0 * amp - amp.T
    trace[...] = lanes(amp * bar)
    bar_h[...], bar_l[...] = split(occ[11] * bar)
    total[...] = before[...] + product((bar_h[...], bar_l[...]), halves, False)
    other = (far_h[...], far_l[...])
    crosses[1 - odd] = product(halves, other, True) / (occ[3] - col - far[...])
    one.wait()
    rows_h[...], rows_l[...] = split(rows[0])
    halves = (rows_h[...], rows_l[...])
    crosses[odd] = product(halves, other, True) / (occ[2] - col - far[...])


def last_far_kernel(pair, which, start, occ, vir, far, high, low, far_rows, crosses, before,
                    total, trace, rows, rows_h, rows_l, bar_h, bar_l, sems):
    size = rows.shape[0]
    rows_copy = load(far_rows, rows, sems.at[0])
    rows_copy.wait()
    rows_h[...], rows_l[...] = split(rows[...])
    halves = (rows_h[...], rows_l[...])
    part = slice(start, start + size)
    gap = occ[pair] - column(vir[...]) - far[:, part]
    amp = product((high[...], low[...]), halves, True) / gap
    bar = 2.0 * amp - crosses[which, :, part]
    trace[...] = lanes(amp * bar)
    bar_h[...], bar_l[...] = split(occ[pair + 8] * bar)
    total[...] = before[...] + product((bar_h[...], bar_l[...]), halves, False)


VMEM = pl.BlockSpec(memory_space=pltpu.VMEM)
SMEM = pl.BlockSpec(memory_space=pltpu.SMEM)
HBM = pl.BlockSpec(memory_space=pltpu.HBM)


def call(kernel, units, inputs, outputs, scratch):
    leaves, tree = jax.tree.flatten(inputs, is_leaf=lambda x: isinstance(x, tuple) and len(x) == 2 and isinstance(x[0], pl.BlockSpec))
    specs = [leaf[0] for leaf in leaves]
    arrays = [leaf[1] for leaf in leaves]
    count = len(arrays)

    def body(*refs):
        ins = jax.tree.unflatten(tree, refs[:count])
        kernel(*ins, *refs[count:])

    return pl.pallas_call(
        body,
        in_specs=specs,
        out_specs=tuple(o[0] for o in outputs),
        out_shape=tuple(jax.ShapeDtypeStruct(o[1], o[2]) for o in outputs),
        scratch_shapes=scratch,
        compiler_params=pltpu.CompilerParams(vmem_limit_bytes=28 * 2**20),
        cost_estimate=pl.CostEstimate(
            flops=int(units * 6 * arrays[-1].size * 512), bytes_accessed=8 << 20, transcendentals=0
        ),
    )(*arrays)


def gathered_plane(factor, occ_energy, vir_energy):
    own = factor[0]
    rows, aux = own.shape
    half = rows // 2
    occs = lax.axis_size("occ")
    me = lax.axis_index("occ")
    odd = me % 2

    def core(value):
        return permuted(value, lambda i, v: (i ^ 1, v))

    def mixed(value, parity):
        return permuted(value, lambda i, v: (i ^ 2, v) if i % 2 == parity else (i, v ^ 1))

    far_vir = permuted(vir_energy, lambda i, v: (i, v ^ 1))
    e = {0: occ_energy[0]}
    for m in (1, 2, 3):
        e[m] = permuted(occ_energy, lambda i, v, m=m: (i ^ m, v))[0]
    near = core(own)
    first = mixed(own, 0)
    own_again, first = lax.optimization_barrier((own, first))
    second = mixed(own_again, 1)
    first_core = core(first)
    low_first, high_first = first[:half], first[half:]
    low_part = mixed(low_first, 1)
    high_part = mixed(high_first, 1)
    second_core = core(second)
    low_core, high_core = core(low_part), core(high_part)

    w0, w1, w2 = weight(0, occs), weight(1, occs), weight(2, occs)
    e1 = jnp.where(odd == 0, e[2], e[3])
    e2 = jnp.where(odd == 0, e[3], e[2])
    wn1 = jnp.where(odd == 0, w2, w1).astype(F32)
    wn2 = jnp.where(odd == 0, w1, w2).astype(F32)
    ef1 = jnp.where(odd == 0, e[1], e[0])
    ef2 = jnp.where(odd == 0, e[0], e[1])
    wf1 = jnp.where(odd == 0, 2 * w1, w0).astype(F32)
    wf2 = jnp.where(odd == 0, w0, 2 * w1).astype(F32)
    pairs = [e[0], e[1], e1, e2, e[2], e[3], ef1, ef2]
    weights = [jnp.asarray(w, F32) for w in (w0, w1, wn1, wn2, w2, w1, wf1, wf2)]
    occ = jnp.stack([e[0] + p for p in pairs] + weights)
    vir, far = vir_energy[None, :], far_vir[None, :]

    block = (rows, aux)
    square = (rows, rows)
    full = pltpu.VMEM(block, F32)
    full_h = pltpu.VMEM(block, BF16)
    bar = pltpu.VMEM(square, BF16)
    sems = pltpu.SemaphoreType.DMA((5,))
    line = (VMEM, (1, rows), F32)
    dense = (VMEM, block, F32)

    high, low, density, trace_own = call(
        own_kernel, 2,
        [(SMEM, occ), (VMEM, vir), (VMEM, own)],
        [(VMEM, block, BF16), (VMEM, block, BF16), dense, line],
        [bar, bar],
    )
    scratch = [full, full_h, full_h, bar, bar, sems]
    density, trace_1n = call(
        functools.partial(near_kernel, 1, False), 2,
        [(SMEM, occ), (VMEM, vir), (VMEM, high), (VMEM, low), (HBM, near), (HBM, near), (VMEM, density)],
        [dense, line], scratch,
    )
    density, trace_n1 = call(
        functools.partial(near_kernel, 2, True), 2,
        [(SMEM, occ), (VMEM, vir), (VMEM, high), (VMEM, low), (HBM, first), (HBM, first_core), (VMEM, density)],
        [dense, line], scratch,
    )
    density, amp_first = call(
        first_far_kernel, 2,
        [(SMEM, occ), (VMEM, vir), (VMEM, far), (VMEM, high), (VMEM, low), (HBM, first_core), (HBM, first), (VMEM, density)],
        [dense, (VMEM, square, F32)], scratch,
    )
    density, trace_0f, trace_1f, far_h, far_l = call(
        second_far_kernel, 4,
        [(SMEM, occ), (VMEM, vir), (VMEM, far), (VMEM, high), (VMEM, low), (HBM, near),
         [(HBM, first_core), (HBM, first)], (HBM, second), (HBM, second_core), (VMEM, amp_first), (VMEM, density)],
        [dense, line, line, (VMEM, block, BF16), (VMEM, block, BF16)],
        [pltpu.VMEM((3, *block), F32), full_h, full_h, pltpu.VMEM((2, *block), BF16), pltpu.VMEM((2, *block), BF16),
         pltpu.VMEM((2, *square), F32), bar, bar, sems],
    )
    density, trace_n2, crosses = call(
        near_cross_kernel, 4,
        [(SMEM, occ), (VMEM, vir), (VMEM, far), (VMEM, high), (VMEM, low), (VMEM, far_h), (VMEM, far_l),
         [(HBM, first), (HBM, first_core)], [(HBM, second_core), (HBM, second)], (VMEM, density)],
        [dense, line, (VMEM, (2, *square), F32)],
        [pltpu.VMEM((2, *block), F32), full_h, full_h, bar, bar, sems],
    )

    part = (half, aux)
    part_bar = pltpu.VMEM((rows, half), BF16)
    scratch = [pltpu.VMEM(part, F32), pltpu.VMEM(part, BF16), pltpu.VMEM(part, BF16),
               part_bar, part_bar, sems]
    last = {2: [], 3: []}
    for start, parts in ((0, (low_part, low_core)), (half, (high_part, high_core))):
        for which, (move, value) in enumerate(zip((2, 3), parts)):
            density, trace = call(
                functools.partial(last_far_kernel, 2 + move, which, start), 1,
                [(SMEM, occ), (VMEM, vir), (VMEM, far), (VMEM, high), (VMEM, low), (HBM, value), (VMEM, crosses), (VMEM, density)],
                [dense, (VMEM, (1, half), F32)], scratch,
            )
            last[move].append(trace)

    trace_near = {0: jnp.sum(trace_own + trace_0f), 1: jnp.sum(trace_1n + trace_1f)}
    sum_n1, sum_n2 = jnp.sum(trace_n1), jnp.sum(trace_n2)
    trace_near[2] = jnp.where(odd == 0, sum_n1, sum_n2) + jnp.sum(last[2][0] + last[2][1])
    trace_near[3] = jnp.where(odd == 0, sum_n2, sum_n1) + jnp.sum(last[3][0] + last[3][1])
    traces = [trace_near[0], jnp.where(odd == 1, trace_near[1], trace_near[3]), trace_near[2]]
    return density[None], jnp.stack(traces)


def contract(pattern, former, latter):
    return jnp.einsum(
        pattern, former, latter, precision=lax.Precision.HIGH, preferred_element_type=F32
    )


def gathered_ring(factor, occ_energy, vir_energy):
    own = factor[0]
    occs = lax.axis_size("occ")
    far_vir = permuted(vir_energy, lambda i, v: (i, v ^ 1))
    own_far = permuted(own, lambda i, v: (i, v ^ 1))
    sums_near = vir_energy[:, None] + vir_energy[None, :]
    sums_far = vir_energy[:, None] + far_vir[None, :]
    density, trace_of = 0.0, {}
    for d in range(occs):
        if weight(d, occs) == 0:
            continue
        near = permuted(own, lambda i, v, d=d: (i - d, v))
        far = permuted(near, lambda i, v: (i, v ^ 1))
        pair = occ_energy[0] + permuted(occ_energy, lambda i, v, d=d: (i - d, v))[0]
        amp_near = contract("ap,bp->ab", own, near) / (pair - sums_near)
        amp_far = contract("ap,bp->ab", own, far) / (pair - sums_far)
        cross = contract("ap,bp->ab", near, own_far) / (pair - sums_far)
        bar_near = 2.0 * amp_near - amp_near.T
        bar_far = 2.0 * amp_far - cross
        density = density + weight(d, occs) * (
            contract("ab,bp->ap", bar_near, near) + contract("ab,bp->ap", bar_far, far)
        )
        trace_of[d] = jnp.sum(amp_near * bar_near) + jnp.sum(amp_far * bar_far)
    return density[None], jnp.stack([trace_of[k % occs] for k in range(STEPS)])


def local(factor, occ_energy, vir_energy):
    gathered = gathered_plane if lax.axis_size("occ") == 4 else gathered_ring
    density, traces = gathered(factor, occ_energy, vir_energy)
    virs = lax.axis_size("vir")
    nvir = factor.shape[1] * virs
    terms = traces[None] / nvir
    if virs > 8:
        return density, lax.psum(terms, "vir")
    others = [permuted(terms, lambda i, v, d=d: (i, v ^ d)) for d in range(1, virs)]
    return density, sum(others, terms)


def solution(mesh):
    placed = (P("occ", "vir", None), P("occ"), P("vir"))
    return jax.shard_map(
        local,
        mesh=mesh,
        in_specs=placed,
        out_specs=(P("occ", "vir", None), P("occ", None)),
        check_vma=False,
    )
```

```python
import functools

import jax
import jax.numpy as jnp
from jax import lax
from jax.experimental import pallas as pl
from jax.experimental.pallas import tpu as pltpu
from jax.sharding import PartitionSpec as P


STEPS = 3
AXES = ("occ", "vir")
F32, BF16 = jnp.float32, jnp.bfloat16
VMEM_LIMIT = 16 * 2**20


def permuted(value, move):
    occs, virs = lax.axis_size("occ"), lax.axis_size("vir")
    route = []
    for i in range(occs):
        for v in range(virs):
            source = move(i, v)
            route.append((source[0] % occs * virs + source[1], i * virs + v))
    return lax.ppermute(value, AXES, route)


def weight(offset, occs):
    return sum(offset == k % occs for k in range(STEPS)) + sum(
        offset == -k % occs for k in range(STEPS)
    )


def split(value):
    high = value.astype(BF16)
    return high, (value - high.astype(F32)).astype(BF16)


def dot(former, latter, transposed):
    contracted = ((1,), (1 if transposed else 0,))
    return lax.dot_general(
        former, latter, (contracted, ((), ())), preferred_element_type=F32
    )


def product(former, latter, transposed):
    (fh, fl), (lh, ll) = former, latter
    return dot(fh, lh, transposed) + dot(fh, ll, transposed) + dot(fl, lh, transposed)


def column(row):
    return jnp.transpose(jnp.broadcast_to(row, (8, row.shape[1])))[:, :1]


def lanes(value):
    return jnp.sum(value, axis=0, keepdims=True)


def is_odd():
    return lax.rem(lax.axis_index("occ"), 2)


def choose(odd, for_even, for_odd):
    pl.when(odd == 0)(for_even)
    pl.when(odd == 1)(for_odd)


def put_split(high, low, value):
    high[...], low[...] = split(value)


def each(rows, body, count=2):
    size = rows // count

    def step(m, carry):
        body(pl.ds(pl.multiple_of(m * size, size), size))
        return carry

    lax.fori_loop(0, count, step, 0)


def own_kernel(occ, vir, rows, high, low, total, traces, col, amp, bar_h, bar_l):
    n = rows.shape[0]
    put_split(high, low, rows[...])
    col[...] = occ[0] - column(vir[...])

    def amps(m):
        amp[m] = product((high[m], low[m]), (high[...], low[...]), True) / (col[m] - vir[...])

    each(n, amps)
    traces[...] = jnp.zeros(traces.shape, F32)
    traces[0:1] = lanes(amp[...] * amp[...])
    put_split(bar_h, bar_l, occ[8] * amp[...])

    def totals(m):
        total[m] = product((bar_h[m], bar_l[m]), (high[...], low[...]), False)

    each(n, totals)


def near_kernel(pair, chosen, occ, vir, high, low, even_rows, odd_rows, before, traces_in,
                total, rows_h, rows_l, traces, col, amp, bar_h, bar_l):
    n = high.shape[0]
    if chosen:
        choose(is_odd(), lambda: put_split(rows_h, rows_l, even_rows[...]),
               lambda: put_split(rows_h, rows_l, odd_rows[...]))
    else:
        put_split(rows_h, rows_l, even_rows[...])
    col[...] = occ[pair] - column(vir[...])

    def amps(m):
        amp[m] = product((high[m], low[m]), (rows_h[...], rows_l[...]), True) / (col[m] - vir[...])

    each(n, amps)
    bar = 2.0 * amp[...] - amp[...].T
    traces[...] = traces_in[...]
    row = 2 + is_odd() if chosen else 1
    traces[pl.ds(row, 1)] = lanes(amp[...] * bar)
    put_split(bar_h, bar_l, occ[pair + 8] * bar)

    def totals(m):
        total[m] = before[m] + product((bar_h[m], bar_l[m]), (rows_h[...], rows_l[...]), False)

    each(n, totals)


def middle_kernel(occ, vir, far, high, low, even_first, odd_first, second,
                  pair_h, pair_l, amps, col):
    odd = is_odd()
    choose(odd, lambda: put_split(pair_h.at[1], pair_l.at[1], even_first[...]),
           lambda: put_split(pair_h.at[0], pair_l.at[0], odd_first[...]))
    put_split(pair_h.at[odd], pair_l.at[odd], second[...])
    col[...] = column(vir[...])
    row_second = jnp.where(odd == 0, far[...], vir[...])
    scale = jnp.where(odd == 0, occ[0], occ[3])

    def step(m):
        left = (high[m], low[m])
        amps[1 - odd, m] = product(left, (pair_h[1 - odd], pair_l[1 - odd]), True) / (
            occ[6] - col[m] - far[...])
        amps[odd, m] = product(left, (pair_h[odd], pair_l[odd]), True) / (
            scale - col[m] - row_second)

    each(high.shape[0], step)


def far_kernel(occ, vir, far, high, low, near_h, near_l, pair_h, pair_l, amps, second_core,
               before, traces_in, total, rest_h, rest_l, rest_amp, traces, col):
    odd = is_odd()
    put_split(rest_h.at[1 - odd], rest_l.at[1 - odd], second_core[...])
    rest_h[odd], rest_l[odd] = pair_h[1], pair_l[1]
    rest_amp[odd] = amps[1]
    col[...] = column(vir[...])
    row_second = jnp.where(odd == 0, vir[...], far[...])
    traces[...] = traces_in[...]
    scale = jnp.where(odd == 0, occ[3], occ[1])

    def step(m):
        rest_amp[1 - odd, m] = product(
            (high[m], low[m]), (rest_h[1 - odd], rest_l[1 - odd]), True) / (scale - col[m] - row_second)
        own_amp = amps[0, m]
        cross = product((near_h[m], near_l[m]), (pair_h[0], pair_l[0]), True) / (
            occ[1] - col[m] - far[...])
        near_amp = rest_amp[0, m]
        bar = 2.0 * near_amp - cross
        traces[0:1] += lanes(own_amp * own_amp)
        traces[1:2] += lanes(near_amp * bar)
        total[m] = (
            before[m]
            + product(split(occ[8] * own_amp), (pair_h[0], pair_l[0]), False)
            + product(split(occ[9] * bar), (rest_h[0], rest_l[0]), False)
        )

    each(high.shape[0], step)


def cross_kernel(occ, vir, far, pair_h, pair_l, rest_h, rest_l, rest_amp, first_h, first_l,
                 before, traces_in, total, crosses, traces, col, bar_h, bar_l):
    odd = is_odd()
    amp = rest_amp[1]
    bar = 2.0 * amp - amp.T
    traces[...] = traces_in[...]
    traces[pl.ds(3 - odd, 1)] = lanes(amp * bar)
    put_split(bar_h, bar_l, occ[11] * bar)
    col[...] = column(vir[...])

    def step(m):
        other = (pair_h[0], pair_l[0])
        crosses[1 - odd, m] = product((rest_h[1, m], rest_l[1, m]), other, True) / (
            occ[3] - col[m] - far[...])
        crosses[odd, m] = product((first_h[m], first_l[m]), other, True) / (
            occ[2] - col[m] - far[...])
        total[m] = before[m] + product((bar_h[m], bar_l[m]), (rest_h[1], rest_l[1]), False)

    each(bar_h.shape[0], step)


def last_kernel(start, final, occ, vir, far, high, low, two_away, three_away, crosses, before,
                traces_in, total, traces, rows_h, rows_l, col, sums):
    size = two_away.shape[0]
    put_split(rows_h.at[:size], rows_l.at[:size], two_away[...])
    put_split(rows_h.at[size:], rows_l.at[size:], three_away[...])
    part = slice(start, start + size)
    col[...] = column(vir[...])
    row = jnp.concatenate([occ[4] - far[:, part], occ[5] - far[:, part]], axis=1)
    lane = lax.broadcasted_iota(jnp.int32, (1, 2 * size), 1)
    scale = jnp.where(lane < size, occ[12], occ[13])
    sums[...] = jnp.zeros(sums.shape, F32)

    def step(m):
        amp = product((high[m], low[m]), (rows_h[...], rows_l[...]), True) / (row - col[m])
        bar = 2.0 * amp - jnp.concatenate([crosses[0, m, part], crosses[1, m, part]], axis=1)
        sums[...] += lanes(amp * bar)
        total[m] = before[m] + product(split(scale * bar), (rows_h[...], rows_l[...]), False)

    each(high.shape[0], step)
    two, three = sums[:, :size], sums[:, size:]
    if not final:
        traces[...] = traces_in[...]
        traces[2:3, :size] += two
        traces[3:4, :size] += three
        return
    odd = is_odd()
    whole = [jnp.sum(traces_in[k : k + 1], axis=1, keepdims=True) for k in range(4)]
    whole[2] += jnp.sum(two, axis=1, keepdims=True)
    whole[3] += jnp.sum(three, axis=1, keepdims=True)
    lane = lax.broadcasted_iota(jnp.int32, (1, 128), 1)
    by_offset = [whole[0], jnp.where(odd == 1, whole[1], whole[3]), whole[2]]
    traces[...] = sum(jnp.where(lane == k, by_offset[k], 0.0) for k in range(3)) * occ[16]


VMEM = pl.BlockSpec(memory_space=pltpu.VMEM)
SMEM = pl.BlockSpec(memory_space=pltpu.SMEM)


def call(kernel, units, inputs, outputs, scratch):
    rows = inputs[1].shape[1]
    return pl.pallas_call(
        kernel,
        in_specs=[SMEM] + [VMEM] * (len(inputs) - 1),
        out_specs=tuple(VMEM for _ in outputs),
        out_shape=tuple(jax.ShapeDtypeStruct(*o) for o in outputs),
        scratch_shapes=scratch,
        compiler_params=pltpu.CompilerParams(vmem_limit_bytes=VMEM_LIMIT),
        cost_estimate=pl.CostEstimate(
            flops=units * 6 * rows * rows * 1024, bytes_accessed=8 << 20, transcendentals=0
        ),
    )(*inputs)


def gathered_plane(factor, occ_energy, vir_energy):
    own = factor[0]
    rows, aux = own.shape
    half = rows // 2
    occs = lax.axis_size("occ")
    me = lax.axis_index("occ")
    odd = me % 2

    def core(value):
        return permuted(value, lambda i, v: (i ^ 1, v))

    def mixed(value, parity):
        return permuted(value, lambda i, v: (i ^ 2, v) if i % 2 == parity else (i, v ^ 1))

    far_vir = permuted(vir_energy, lambda i, v: (i, v ^ 1))
    e = {0: occ_energy[0]}
    for m in (1, 2, 3):
        e[m] = permuted(occ_energy, lambda i, v, m=m: (i ^ m, v))[0]
    near = core(own)
    first = mixed(own, 0)
    own_again, first = lax.optimization_barrier((own, first))
    second = mixed(own_again, 1)
    first_core = core(first)
    low_first, high_first = first[:half], first[half:]
    low_part = mixed(low_first, 1)
    high_part = mixed(high_first, 1)
    second_core = core(second)
    low_core, high_core = core(low_part), core(high_part)

    w0, w1, w2 = weight(0, occs), weight(1, occs), weight(2, occs)
    e1 = jnp.where(odd == 0, e[2], e[3])
    e2 = jnp.where(odd == 0, e[3], e[2])
    wn1 = jnp.where(odd == 0, w2, w1).astype(F32)
    wn2 = jnp.where(odd == 0, w1, w2).astype(F32)
    ef1 = jnp.where(odd == 0, e[1], e[0])
    pairs = [e[0], e[1], e1, e2, e[2], e[3], ef1, e[0]]
    weights = [jnp.asarray(w, F32) for w in (w0, w1, wn1, wn2, w2, w1, 0, 0)]
    count = rows * lax.axis_size("vir")
    weights.append(jnp.full((), 1 / count, F32))
    occ = jnp.stack([e[0] + p for p in pairs] + weights)
    occ_core = jnp.stack([e[0] + e[0], e[0] + e[1]] + weights[:6] + weights)
    occ_own = jnp.stack([e[0] + e[0]] + weights[:7] + weights)
    vir, far = vir_energy[None, :], far_vir[None, :]

    block, square = (rows, aux), (rows, rows)
    bar = pltpu.VMEM(square, BF16)
    col = pltpu.VMEM((rows, 1), F32)
    amp = pltpu.VMEM(square, F32)
    dense = (block, F32)
    halves = [(block, BF16), (block, BF16)]
    doubles = [((2, *block), BF16), ((2, *block), BF16)]
    amps_out = ((2, *square), F32)
    lines = ((8, rows), F32)

    high, low, density, traces = call(
        own_kernel, 2, [occ_own, vir, own], [*halves, dense, lines], [col, amp, bar, bar])
    density, near_h, near_l, traces = call(
        functools.partial(near_kernel, 1, False), 2,
        [occ_core, vir, high, low, near, near, density, traces], [dense, *halves, lines], [col, amp, bar, bar])
    density, first_h, first_l, traces = call(
        functools.partial(near_kernel, 2, True), 2,
        [occ, vir, high, low, first, first_core, density, traces], [dense, *halves, lines], [col, amp, bar, bar])
    pair_h, pair_l, amps = call(
        middle_kernel, 2,
        [occ, vir, far, high, low, first_core, first, second], [*doubles, amps_out], [col])
    density, rest_h, rest_l, rest_amp, traces = call(
        far_kernel, 4,
        [occ, vir, far, high, low, near_h, near_l, pair_h, pair_l, amps, second_core, density, traces],
        [dense, *doubles, amps_out, lines], [col])
    density, crosses, traces = call(
        cross_kernel, 3,
        [occ, vir, far, pair_h, pair_l, rest_h, rest_l, rest_amp, first_h, first_l, density, traces],
        [dense, amps_out, lines], [col, bar, bar])
    sums = pltpu.VMEM((1, 2 * half), F32)
    scratch = [pltpu.VMEM((2 * half, aux), BF16), pltpu.VMEM((2 * half, aux), BF16), col, sums]
    density, traces = call(
        functools.partial(last_kernel, 0, False), 2,
        [occ, vir, far, high, low, low_part, low_core, crosses, density, traces], [dense, lines], scratch)
    density, traces = call(
        functools.partial(last_kernel, half, True), 2,
        [occ, vir, far, high, low, high_part, high_core, crosses, density, traces],
        [dense, ((1, 128), F32)], scratch)
    return density[None], traces


def contract(pattern, former, latter):
    return jnp.einsum(
        pattern, former, latter, precision=lax.Precision.HIGH, preferred_element_type=F32
    )


def gathered_ring(factor, occ_energy, vir_energy):
    own = factor[0]
    occs = lax.axis_size("occ")
    far_vir = permuted(vir_energy, lambda i, v: (i, v ^ 1))
    own_far = permuted(own, lambda i, v: (i, v ^ 1))
    sums_near = vir_energy[:, None] + vir_energy[None, :]
    sums_far = vir_energy[:, None] + far_vir[None, :]
    density, trace_of = 0.0, {}
    for d in range(occs):
        if weight(d, occs) == 0:
            continue
        near = permuted(own, lambda i, v, d=d: (i - d, v))
        far = permuted(near, lambda i, v: (i, v ^ 1))
        pair = occ_energy[0] + permuted(occ_energy, lambda i, v, d=d: (i - d, v))[0]
        amp_near = contract("ap,bp->ab", own, near) / (pair - sums_near)
        amp_far = contract("ap,bp->ab", own, far) / (pair - sums_far)
        cross = contract("ap,bp->ab", near, own_far) / (pair - sums_far)
        bar_near = 2.0 * amp_near - amp_near.T
        bar_far = 2.0 * amp_far - cross
        density = density + weight(d, occs) * (
            contract("ab,bp->ap", bar_near, near) + contract("ab,bp->ap", bar_far, far)
        )
        trace_of[d] = jnp.sum(amp_near * bar_near) + jnp.sum(amp_far * bar_far)
    return density[None], jnp.stack([trace_of[k % occs] for k in range(STEPS)])


def local(factor, occ_energy, vir_energy):
    gathered = gathered_plane if lax.axis_size("occ") == 4 else gathered_ring
    density, traces = gathered(factor, occ_energy, vir_energy)
    virs = lax.axis_size("vir")
    nvir = factor.shape[1] * virs
    if gathered is gathered_ring:
        return density, lax.psum(traces[None] / nvir, "vir")
    apart = 1
    while apart < virs:
        traces = traces + permuted(traces, lambda i, v: (i, v ^ apart))
        apart *= 2
    return density, traces[:, :STEPS]


def solution(mesh):
    placed = (P("occ", "vir", None), P("occ"), P("vir"))
    return jax.shard_map(
        local,
        mesh=mesh,
        in_specs=placed,
        out_specs=(P("occ", "vir", None), P("occ", None)),
        check_vma=False,
    )
```

```python
import functools

import jax
import jax.numpy as jnp
from jax import lax
from jax.experimental import pallas as pl
from jax.experimental.pallas import tpu as pltpu
from jax.sharding import PartitionSpec as P


STEPS = 3
AXES = ("occ", "vir")
F32, BF16 = jnp.float32, jnp.bfloat16
VMEM_LIMIT = 12 * 2**20


def permuted(value, move):
    occs, virs = lax.axis_size("occ"), lax.axis_size("vir")
    route = []
    for i in range(occs):
        for v in range(virs):
            source = move(i, v)
            route.append((source[0] % occs * virs + source[1], i * virs + v))
    return lax.ppermute(value, AXES, route)


def weight(offset, occs):
    return sum(offset == k % occs for k in range(STEPS)) + sum(
        offset == -k % occs for k in range(STEPS)
    )


def split(value):
    high = value.astype(BF16)
    return high, (value - high.astype(F32)).astype(BF16)


def dot(former, latter, transposed):
    contracted = ((1,), (1 if transposed else 0,))
    return lax.dot_general(
        former, latter, (contracted, ((), ())), preferred_element_type=F32
    )


def product(former, latter, transposed):
    (fh, fl), (lh, ll) = former, latter
    return dot(fh, lh, transposed) + dot(fh, ll, transposed) + dot(fl, lh, transposed)


def column(row):
    return jnp.transpose(jnp.broadcast_to(row, (8, row.shape[1])))[:, :1]


def lanes(value):
    return jnp.sum(value, axis=0, keepdims=True)


def is_odd():
    return lax.rem(lax.axis_index("occ"), 2)


def each(rows, body, count=2):
    size = rows // count

    def step(m, carry):
        body(pl.ds(pl.multiple_of(m * size, size), size))
        return carry

    lax.fori_loop(0, count, step, 0)


def put_split(high, low, rows):
    def step(m):
        high[m], low[m] = split(rows[m])

    each(rows.shape[0], step, 4)


def start_kernel(weights, e0, e1, vir, own, near, total, blocks_h, blocks_l, traces,
                 col, amp, bar_h, bar_l):
    n = own.shape[0]
    put_split(blocks_h.at[0], blocks_l.at[0], own)
    put_split(blocks_h.at[1], blocks_l.at[1], near)
    total[...] = jnp.zeros(total.shape, F32)
    traces[...] = jnp.zeros(traces.shape, F32)

    def block(k, carry):
        pair = e0[0] + jnp.where(k == 0, e0[0], e1[0])
        scale = jnp.where(k == 0, float(weights[0]), float(weights[1]))
        col[...] = pair - column(vir[...])

        def amps(m):
            amp[m] = product((blocks_h[0, m], blocks_l[0, m]), (blocks_h[k], blocks_l[k]), True) / (
                col[m] - vir[...])

        each(n, amps)
        bar = 2.0 * amp[...] - amp[...].T
        traces[pl.ds(k, 1)] = lanes(amp[...] * bar)
        bar_h[...], bar_l[...] = split(scale * bar)

        def totals(m):
            total[m] += product((bar_h[m], bar_l[m]), (blocks_h[k], blocks_l[k]), False)

        each(n, totals)
        return carry

    lax.fori_loop(0, 2, block, 0)


def first_kernel(weights, e0, e1, e2, e3, vir, far, blocks_h, blocks_l, first, first_core, before,
                 traces_in, total, firsts_h, firsts_l, far_amp, traces, col, amp, bar_h, bar_l):
    n = first.shape[0]
    odd = is_odd()
    put_split(firsts_h.at[0], firsts_l.at[0], first)
    put_split(firsts_h.at[1], firsts_l.at[1], first_core)
    pair = e0[0] + jnp.where(odd == 0, e2[0], e3[0])
    pair_far = e0[0] + jnp.where(odd == 0, e1[0], e0[0])
    scale = jnp.where(odd == 0, float(weights[2]), float(weights[1]))
    col[...] = column(vir[...])

    def amps(m):
        left = (blocks_h[0, m], blocks_l[0, m])
        amp[m] = product(left, (firsts_h[odd], firsts_l[odd]), True) / (pair - col[m] - vir[...])
        far_amp[m] = product(left, (firsts_h[1 - odd], firsts_l[1 - odd]), True) / (
            pair_far - col[m] - far[...])

    each(n, amps)
    bar = 2.0 * amp[...] - amp[...].T
    traces[...] = traces_in[...]
    traces[pl.ds(2 + odd, 1)] = lanes(amp[...] * bar)
    bar_h[...], bar_l[...] = split(scale * bar)

    def totals(m):
        total[m] = before[m] + product((bar_h[m], bar_l[m]), (firsts_h[odd], firsts_l[odd]), False)

    each(n, totals)


def middle_kernel(e0, e2, vir, far, blocks_h, blocks_l, firsts_h, firsts_l, far_amp, second,
                  pair_h, pair_l, amps, col):
    n = second.shape[0]
    odd = is_odd()
    put_split(pair_h.at[odd], pair_l.at[odd], second)
    pair_h[1 - odd], pair_l[1 - odd] = firsts_h[1 - odd], firsts_l[1 - odd]
    amps[1 - odd] = far_amp[...]
    col[...] = column(vir[...])
    row = jnp.where(odd == 0, far[...], vir[...])
    pair = e0[0] + jnp.where(odd == 0, e0[0], e2[0])

    def step(m):
        amps[odd, m] = product(
            (blocks_h[0, m], blocks_l[0, m]), (pair_h[odd], pair_l[odd]), True) / (pair - col[m] - row)

    each(n, step)


def amps_kernel(weights, e0, e1, e2, e3, vir, far, blocks_h, blocks_l, pair_h, pair_l, amps,
                firsts_h, firsts_l, second_core, traces_in,
                rest_h, rest_l, bars_h, bars_l, crosses, traces, rest_amp, col):
    n = second_core.shape[0]
    odd = is_odd()
    put_split(rest_h.at[1 - odd], rest_l.at[1 - odd], second_core)
    rest_h[odd], rest_l[odd] = pair_h[1], pair_l[1]
    rest_amp[odd] = amps[1]
    col[...] = column(vir[...])
    row = jnp.where(odd == 0, vir[...], far[...])
    pair = e0[0] + jnp.where(odd == 0, e3[0], e1[0])
    pair_first = e0[0] + jnp.where(odd == 0, e2[0], e3[0])
    pair_second = e0[0] + jnp.where(odd == 0, e3[0], e2[0])
    traces[...] = traces_in[...]

    def step(m):
        other = (pair_h[0], pair_l[0])
        sums = col[m] + far[...]
        rest_amp[1 - odd, m] = product(
            (blocks_h[0, m], blocks_l[0, m]), (rest_h[1 - odd], rest_l[1 - odd]), True) / (
                pair - col[m] - row)
        own_amp = amps[0, m]
        bars_h[0, m], bars_l[0, m] = split(float(weights[0]) * own_amp)
        cross = product((blocks_h[1, m], blocks_l[1, m]), other, True) / (e0[0] + e1[0] - sums)
        near_amp = rest_amp[0, m]
        bar = 2.0 * near_amp - cross
        traces[0:1] += lanes(own_amp * own_amp)
        traces[1:2] += lanes(near_amp * bar)
        bars_h[1, m], bars_l[1, m] = split(float(weights[1]) * bar)
        crosses[1 - odd, m] = product((rest_h[1, m], rest_l[1, m]), other, True) / (pair_second - sums)
        crosses[odd, m] = product((firsts_h[odd, m], firsts_l[odd, m]), other, True) / (pair_first - sums)

    each(n, step)
    amp = rest_amp[1]
    bar = 2.0 * amp - amp.T
    traces[pl.ds(3 - odd, 1)] = lanes(amp * bar)
    scale = jnp.where(odd == 0, float(weights[1]), float(weights[2]))
    bars_h[2], bars_l[2] = split(scale * bar)


def add_kernel(terms, before, *refs):
    total = refs[-1]

    def at(ref, slot, m=slice(None)):
        return ref[m] if slot is None else ref[slot, m]

    def step(m):
        value = before[m]
        for k, (bar, block) in enumerate(terms):
            bar_h, bar_l, block_h, block_l = refs[4 * k : 4 * k + 4]
            value += product((at(bar_h, bar, m), at(bar_l, bar, m)), (at(block_h, block), at(block_l, block)), False)
        total[m] = value

    each(before.shape[0], step)


def part_kernel(weights, start, factor, e0, e2, e3, vir, far, blocks_h, blocks_l, two_away, three_away,
                crosses, traces_in, rows_h, rows_l, bar_h, bar_l, traces, col, sums):
    size = two_away.shape[0]
    put_split(rows_h.at[:size], rows_l.at[:size], two_away)
    put_split(rows_h.at[size:], rows_l.at[size:], three_away)
    part = slice(start, start + size)
    col[...] = column(vir[...])
    row = jnp.concatenate([e0[0] + e2[0] - far[:, part], e0[0] + e3[0] - far[:, part]], axis=1)
    lane = lax.broadcasted_iota(jnp.int32, (1, 2 * size), 1)
    scale = jnp.where(lane < size, float(weights[2]), float(weights[1]))
    sums[...] = jnp.zeros(sums.shape, F32)

    def step(m):
        amp = product((blocks_h[0, m], blocks_l[0, m]), (rows_h[...], rows_l[...]), True) / (row - col[m])
        bar = 2.0 * amp - jnp.concatenate([crosses[0, m, part], crosses[1, m, part]], axis=1)
        sums[...] += lanes(amp * bar)
        bar_h[m], bar_l[m] = split(scale * bar)

    each(col.shape[0], step)
    two, three = sums[:, :size], sums[:, size:]
    if factor is None:
        traces[...] = traces_in[...]
        traces[2:3, :size] += two
        traces[3:4, :size] += three
        return
    odd = is_odd()
    whole = [jnp.sum(traces_in[k : k + 1], axis=1, keepdims=True) for k in range(4)]
    whole[2] += jnp.sum(two, axis=1, keepdims=True)
    whole[3] += jnp.sum(three, axis=1, keepdims=True)
    lane = lax.broadcasted_iota(jnp.int32, (1, 128), 1)
    by_offset = [whole[0], jnp.where(odd == 1, whole[1], whole[3]), whole[2]]
    traces[...] = sum(jnp.where(lane == k, by_offset[k], 0.0) for k in range(3)) * factor


VMEM = pl.BlockSpec(memory_space=pltpu.VMEM)
SMEM = pl.BlockSpec(memory_space=pltpu.SMEM)


def call(kernel, units, inputs, outputs, scratch):
    rows = outputs[0][0][-2]
    return pl.pallas_call(
        kernel,
        in_specs=[SMEM if value.size == 1 else VMEM for value in inputs],
        out_specs=tuple(VMEM for _ in outputs),
        out_shape=tuple(jax.ShapeDtypeStruct(*o) for o in outputs),
        scratch_shapes=scratch,
        compiler_params=pltpu.CompilerParams(vmem_limit_bytes=VMEM_LIMIT),
        cost_estimate=pl.CostEstimate(
            flops=units * 6 * rows * rows * 1280, bytes_accessed=8 << 20, transcendentals=0
        ),
    )(*inputs)


def gathered_plane(factor, occ_energy, vir_energy):
    own = factor[0]
    rows, aux = own.shape
    half = rows // 2
    occs = lax.axis_size("occ")

    def core(value):
        return permuted(value, lambda i, v: (i ^ 1, v))

    def mixed(value, parity):
        return permuted(value, lambda i, v: (i ^ 2, v) if i % 2 == parity else (i, v ^ 1))

    far_vir = permuted(vir_energy, lambda i, v: (i, v ^ 1))
    e0 = occ_energy
    e1, e2, e3 = (permuted(e0, lambda i, v, m=m: (i ^ m, v)) for m in (1, 2, 3))
    near = core(own)
    first = mixed(own, 0)
    second = mixed(own, 1)
    first_core = core(first)
    low_first, high_first = first[:half], first[half:]
    low_part = mixed(low_first, 1)
    high_part = mixed(high_first, 1)
    second_core = core(second)
    low_core, high_core = core(low_part), core(high_part)

    weights = [weight(d, occs) for d in range(3)]
    vir, far = vir_energy[None, :], far_vir[None, :]

    block, square = (rows, aux), (rows, rows)
    dense = (block, F32)
    doubles = [((2, *block), BF16)] * 2
    lines = ((8, rows), F32)
    bar = pltpu.VMEM(square, BF16)
    col = pltpu.VMEM((rows, 1), F32)
    amp = pltpu.VMEM(square, F32)
    sums = pltpu.VMEM((1, 2 * half), F32)

    density, *blocks, traces = call(
        functools.partial(start_kernel, weights), 4,
        [e0, e1, vir, own, near], [dense, *doubles, lines], [col, amp, bar, bar])
    density, *firsts, far_amp, traces = call(
        functools.partial(first_kernel, weights), 3,
        [e0, e1, e2, e3, vir, far, *blocks, first, first_core, density, traces],
        [dense, *doubles, (square, F32), lines], [col, amp, bar, bar])
    *pair, amps = call(
        middle_kernel, 1,
        [e0, e2, vir, far, *blocks, *firsts, far_amp, second], [*doubles, ((2, *square), F32)], [col])
    *rest, bars_h, bars_l, crosses, traces = call(
        functools.partial(amps_kernel, weights), 4,
        [e0, e1, e2, e3, vir, far, *blocks, *pair, amps, *firsts, second_core, traces],
        [*doubles, ((3, *square), BF16), ((3, *square), BF16), ((2, *square), F32), lines],
        [pltpu.VMEM((2, *square), F32), col])

    def add(before, *terms):
        slots = tuple((bar_slot, block_slot) for bar_slot, _, block_slot, _ in terms)
        arrays = [array for _, some_bars, _, some_blocks in terms for array in (*some_bars, *some_blocks)]
        return call(
            functools.partial(add_kernel, slots), len(terms), [before, *arrays], [dense], [])[0]

    def part(start, factor, two_away, three_away, traces):
        out = lines if factor is None else ((1, 128), F32)
        *parts, bar_h, bar_l, traces = call(
            functools.partial(part_kernel, weights, start, factor), 1,
            [e0, e2, e3, vir, far, *blocks, two_away, three_away, crosses, traces],
            [((2 * half, aux), BF16)] * 2 + [((rows, 2 * half), BF16)] * 2 + [out], [col, sums])
        return parts, (bar_h, bar_l), traces

    all_bars = (bars_h, bars_l)
    density = add(density, (0, all_bars, 0, pair), (1, all_bars, 0, rest))
    part_0, part_bars_0, traces = part(0, None, low_part, low_core, traces)
    density = add(density, (2, all_bars, 1, rest))
    density = add(density, (None, part_bars_0, None, part_0))
    scale = 1.0 / (rows * lax.axis_size("vir"))
    part_1, part_bars_1, traces = part(half, scale, high_part, high_core, traces)
    density = add(density, (None, part_bars_1, None, part_1))
    return density[None], traces


def contract(pattern, former, latter):
    return jnp.einsum(
        pattern, former, latter, precision=lax.Precision.HIGH, preferred_element_type=F32
    )


def gathered_ring(factor, occ_energy, vir_energy):
    own = factor[0]
    occs = lax.axis_size("occ")
    far_vir = permuted(vir_energy, lambda i, v: (i, v ^ 1))
    own_far = permuted(own, lambda i, v: (i, v ^ 1))
    sums_near = vir_energy[:, None] + vir_energy[None, :]
    sums_far = vir_energy[:, None] + far_vir[None, :]
    density, trace_of = 0.0, {}
    for d in range(occs):
        if weight(d, occs) == 0:
            continue
        near = permuted(own, lambda i, v, d=d: (i - d, v))
        far = permuted(near, lambda i, v: (i, v ^ 1))
        pair = occ_energy[0] + permuted(occ_energy, lambda i, v, d=d: (i - d, v))[0]
        amp_near = contract("ap,bp->ab", own, near) / (pair - sums_near)
        amp_far = contract("ap,bp->ab", own, far) / (pair - sums_far)
        cross = contract("ap,bp->ab", near, own_far) / (pair - sums_far)
        bar_near = 2.0 * amp_near - amp_near.T
        bar_far = 2.0 * amp_far - cross
        density = density + weight(d, occs) * (
            contract("ab,bp->ap", bar_near, near) + contract("ab,bp->ap", bar_far, far)
        )
        trace_of[d] = jnp.sum(amp_near * bar_near) + jnp.sum(amp_far * bar_far)
    return density[None], jnp.stack([trace_of[k % occs] for k in range(STEPS)])


def local(factor, occ_energy, vir_energy):
    gathered = gathered_plane if lax.axis_size("occ") == 4 else gathered_ring
    density, traces = gathered(factor, occ_energy, vir_energy)
    virs = lax.axis_size("vir")
    nvir = factor.shape[1] * virs
    if gathered is gathered_ring:
        return density, lax.psum(traces[None] / nvir, "vir")
    apart = 1
    while apart < virs:
        traces = traces + permuted(traces, lambda i, v: (i, v ^ apart))
        apart *= 2
    return density, traces[:, :STEPS]


def solution(mesh):
    placed = (P("occ", "vir", None), P("occ"), P("vir"))
    return jax.shard_map(
        local,
        mesh=mesh,
        in_specs=placed,
        out_specs=(P("occ", "vir", None), P("occ", None)),
        check_vma=False,
    )
```

```python
import functools

import jax
import jax.numpy as jnp
from jax import lax
from jax.experimental import pallas as pl
from jax.experimental.pallas import tpu as pltpu
from jax.sharding import PartitionSpec as P


STEPS = 3
AXES = ("occ", "vir")
F32, BF16 = jnp.float32, jnp.bfloat16
VMEM_LIMIT = 12 * 2**20


def permuted(value, move):
    occs, virs = lax.axis_size("occ"), lax.axis_size("vir")
    route = []
    for i in range(occs):
        for v in range(virs):
            source = move(i, v)
            route.append((source[0] % occs * virs + source[1], i * virs + v))
    return lax.ppermute(value, AXES, route)


def weight(offset, occs):
    return sum(offset == k % occs for k in range(STEPS)) + sum(
        offset == -k % occs for k in range(STEPS)
    )


def split(value):
    high = value.astype(BF16)
    return high, (value - high.astype(F32)).astype(BF16)


def dot(former, latter, transposed):
    contracted = ((1,), (1 if transposed else 0,))
    return lax.dot_general(
        former, latter, (contracted, ((), ())), preferred_element_type=F32
    )


def product(former, latter, transposed):
    (fh, fl), (lh, ll) = former, latter
    return dot(fh, lh, transposed) + dot(fh, ll, transposed) + dot(fl, lh, transposed)


def column(row):
    return jnp.transpose(jnp.broadcast_to(row, (8, row.shape[1])))[:, :1]


def lanes(value):
    return jnp.sum(value, axis=0, keepdims=True)


def is_odd():
    return lax.rem(lax.axis_index("occ"), 2)


def each(rows, body, count=2):
    size = rows // count

    def step(m, carry):
        body(pl.ds(pl.multiple_of(m * size, size), size))
        return carry

    lax.fori_loop(0, count, step, 0)


def put_split(high, low, rows):
    def step(m):
        high[m], low[m] = split(rows[m])

    each(rows.shape[0], step, 4)


def start_kernel(weights, e0, e1, vir, own, near, total, blocks_h, blocks_l, traces,
                 col, amp, bar_h, bar_l):
    n = own.shape[0]
    put_split(blocks_h.at[0], blocks_l.at[0], own)
    put_split(blocks_h.at[1], blocks_l.at[1], near)
    total[...] = jnp.zeros(total.shape, F32)
    traces[...] = jnp.zeros(traces.shape, F32)

    def block(k, carry):
        pair = e0[0] + jnp.where(k == 0, e0[0], e1[0])
        scale = jnp.where(k == 0, float(weights[0]), float(weights[1]))
        col[...] = pair - column(vir[...])

        def amps(m):
            amp[m] = product((blocks_h[0, m], blocks_l[0, m]), (blocks_h[k], blocks_l[k]), True) / (
                col[m] - vir[...])

        each(n, amps)
        bar = 2.0 * amp[...] - amp[...].T
        traces[pl.ds(k, 1)] = lanes(amp[...] * bar)
        bar_h[...], bar_l[...] = split(scale * bar)

        def totals(m):
            total[m] += product((bar_h[m], bar_l[m]), (blocks_h[k], blocks_l[k]), False)

        each(n, totals)
        return carry

    lax.fori_loop(0, 2, block, 0)


def first_kernel(weights, e0, e1, e2, e3, vir, far, blocks_h, blocks_l, first, first_core, before,
                 traces_in, total, firsts_h, firsts_l, far_amp, traces, col, amp, bar_h, bar_l):
    n = first.shape[0]
    odd = is_odd()
    put_split(firsts_h.at[0], firsts_l.at[0], first)
    put_split(firsts_h.at[1], firsts_l.at[1], first_core)
    pair = e0[0] + jnp.where(odd == 0, e2[0], e3[0])
    pair_far = e0[0] + jnp.where(odd == 0, e1[0], e0[0])
    scale = jnp.where(odd == 0, float(weights[2]), float(weights[1]))
    col[...] = column(vir[...])

    def amps(m):
        left = (blocks_h[0, m], blocks_l[0, m])
        amp[m] = product(left, (firsts_h[odd], firsts_l[odd]), True) / (pair - col[m] - vir[...])
        far_amp[m] = product(left, (firsts_h[1 - odd], firsts_l[1 - odd]), True) / (
            pair_far - col[m] - far[...])

    each(n, amps)
    bar = 2.0 * amp[...] - amp[...].T
    traces[...] = traces_in[...]
    traces[pl.ds(2 + odd, 1)] = lanes(amp[...] * bar)
    bar_h[...], bar_l[...] = split(scale * bar)

    def totals(m):
        total[m] = before[m] + product((bar_h[m], bar_l[m]), (firsts_h[odd], firsts_l[odd]), False)

    each(n, totals)


def middle_kernel(e0, e2, vir, far, blocks_h, blocks_l, firsts_h, firsts_l, far_amp, second,
                  pair_h, pair_l, amps, col):
    n = second.shape[0]
    odd = is_odd()
    put_split(pair_h.at[odd], pair_l.at[odd], second)
    pair_h[1 - odd], pair_l[1 - odd] = firsts_h[1 - odd], firsts_l[1 - odd]
    amps[1 - odd] = far_amp[...]
    col[...] = column(vir[...])
    row = jnp.where(odd == 0, far[...], vir[...])
    pair = e0[0] + jnp.where(odd == 0, e0[0], e2[0])

    def step(m):
        amps[odd, m] = product(
            (blocks_h[0, m], blocks_l[0, m]), (pair_h[odd], pair_l[odd]), True) / (pair - col[m] - row)

    each(n, step)


def amps_kernel(weights, e0, e1, e2, e3, vir, far, blocks_h, blocks_l, pair_h, pair_l, amps,
                firsts_h, firsts_l, second_core, traces_in,
                rest_h, rest_l, bars_h, bars_l, crosses, traces, rest_amp, col):
    n = second_core.shape[0]
    odd = is_odd()
    put_split(rest_h.at[1 - odd], rest_l.at[1 - odd], second_core)
    rest_h[odd], rest_l[odd] = pair_h[1], pair_l[1]
    rest_amp[odd] = amps[1]
    col[...] = column(vir[...])
    row = jnp.where(odd == 0, vir[...], far[...])
    pair = e0[0] + jnp.where(odd == 0, e3[0], e1[0])
    pair_first = e0[0] + jnp.where(odd == 0, e2[0], e3[0])
    pair_second = e0[0] + jnp.where(odd == 0, e3[0], e2[0])
    traces[...] = traces_in[...]

    def step(m):
        other = (pair_h[0], pair_l[0])
        sums = col[m] + far[...]
        rest_amp[1 - odd, m] = product(
            (blocks_h[0, m], blocks_l[0, m]), (rest_h[1 - odd], rest_l[1 - odd]), True) / (
                pair - col[m] - row)
        own_amp = amps[0, m]
        bars_h[0, m], bars_l[0, m] = split(float(weights[0]) * own_amp)
        cross = product((blocks_h[1, m], blocks_l[1, m]), other, True) / (e0[0] + e1[0] - sums)
        near_amp = rest_amp[0, m]
        bar = 2.0 * near_amp - cross
        traces[0:1] += lanes(own_amp * own_amp)
        traces[1:2] += lanes(near_amp * bar)
        bars_h[1, m], bars_l[1, m] = split(float(weights[1]) * bar)
        crosses[1 - odd, m] = product((rest_h[1, m], rest_l[1, m]), other, True) / (pair_second - sums)
        crosses[odd, m] = product((firsts_h[odd, m], firsts_l[odd, m]), other, True) / (pair_first - sums)

    each(n, step)
    amp = rest_amp[1]
    bar = 2.0 * amp - amp.T
    traces[pl.ds(3 - odd, 1)] = lanes(amp * bar)
    scale = jnp.where(odd == 0, float(weights[1]), float(weights[2]))
    bars_h[2], bars_l[2] = split(scale * bar)


def add_kernel(terms, before, *refs):
    total = refs[-1]

    def step(m):
        value = before[m]
        for k, (bar, block, span) in enumerate(terms):
            bar_h, bar_l, block_h, block_l = refs[4 * k : 4 * k + 4]
            left = tuple(ref[m, span] if bar is None else ref[bar, m, span] for ref in (bar_h, bar_l))
            right = tuple(ref[span] if block is None else ref[block, span] for ref in (block_h, block_l))
            value += product(left, right, False)
        total[m] = value

    each(before.shape[0], step)


def part_kernel(weights, start, factor, e0, e2, e3, vir, far, blocks_h, blocks_l, two_away, three_away,
                crosses, traces_in, rows_h, rows_l, bar_h, bar_l, traces, col, sums):
    size = two_away.shape[0]
    put_split(rows_h.at[:size], rows_l.at[:size], two_away)
    put_split(rows_h.at[size:], rows_l.at[size:], three_away)
    part = slice(start, start + size)
    col[...] = column(vir[...])
    row = jnp.concatenate([e0[0] + e2[0] - far[:, part], e0[0] + e3[0] - far[:, part]], axis=1)
    lane = lax.broadcasted_iota(jnp.int32, (1, 2 * size), 1)
    scale = jnp.where(lane < size, float(weights[2]), float(weights[1]))
    sums[...] = jnp.zeros(sums.shape, F32)

    def step(m):
        amp = product((blocks_h[0, m], blocks_l[0, m]), (rows_h[...], rows_l[...]), True) / (row - col[m])
        bar = 2.0 * amp - jnp.concatenate([crosses[0, m, part], crosses[1, m, part]], axis=1)
        sums[...] += lanes(amp * bar)
        bar_h[m], bar_l[m] = split(scale * bar)

    each(col.shape[0], step)
    two, three = sums[:, :size], sums[:, size:]
    if factor is None:
        traces[...] = traces_in[...]
        traces[2:3, :size] += two
        traces[3:4, :size] += three
        return
    odd = is_odd()
    whole = [jnp.sum(traces_in[k : k + 1], axis=1, keepdims=True) for k in range(4)]
    whole[2] += jnp.sum(two, axis=1, keepdims=True)
    whole[3] += jnp.sum(three, axis=1, keepdims=True)
    lane = lax.broadcasted_iota(jnp.int32, (1, 128), 1)
    by_offset = [whole[0], jnp.where(odd == 1, whole[1], whole[3]), whole[2]]
    traces[...] = sum(jnp.where(lane == k, by_offset[k], 0.0) for k in range(3)) * factor


VMEM = pl.BlockSpec(memory_space=pltpu.VMEM)
SMEM = pl.BlockSpec(memory_space=pltpu.SMEM)


def call(kernel, units, inputs, outputs, scratch):
    rows = outputs[0][0][-2]
    return pl.pallas_call(
        kernel,
        in_specs=[SMEM if value.size == 1 else VMEM for value in inputs],
        out_specs=tuple(VMEM for _ in outputs),
        out_shape=tuple(jax.ShapeDtypeStruct(*o) for o in outputs),
        scratch_shapes=scratch,
        compiler_params=pltpu.CompilerParams(vmem_limit_bytes=VMEM_LIMIT),
        cost_estimate=pl.CostEstimate(
            flops=units * 6 * rows * rows * 1280, bytes_accessed=8 << 20, transcendentals=0
        ),
    )(*inputs)


def gathered_plane(factor, occ_energy, vir_energy):
    own = factor[0]
    rows, aux = own.shape
    half = rows // 2
    occs = lax.axis_size("occ")

    def core(value):
        return permuted(value, lambda i, v: (i ^ 1, v))

    def mixed(value, parity):
        return permuted(value, lambda i, v: (i ^ 2, v) if i % 2 == parity else (i, v ^ 1))

    far_vir = permuted(vir_energy, lambda i, v: (i, v ^ 1))
    e0 = occ_energy
    e1, e2, e3 = (permuted(e0, lambda i, v, m=m: (i ^ m, v)) for m in (1, 2, 3))
    near = core(own)
    first = mixed(own, 0)
    second = mixed(own, 1)
    first_core = core(first)
    low_first, high_first = first[:half], first[half:]
    low_part = mixed(low_first, 1)
    high_part = mixed(high_first, 1)
    second_core = core(second)
    low_core, high_core = core(low_part), core(high_part)

    weights = [weight(d, occs) for d in range(3)]
    vir, far = vir_energy[None, :], far_vir[None, :]

    block, square = (rows, aux), (rows, rows)
    dense = (block, F32)
    doubles = [((2, *block), BF16)] * 2
    lines = ((8, rows), F32)
    bar = pltpu.VMEM(square, BF16)
    col = pltpu.VMEM((rows, 1), F32)
    amp = pltpu.VMEM(square, F32)
    sums = pltpu.VMEM((1, 2 * half), F32)

    density, *blocks, traces = call(
        functools.partial(start_kernel, weights), 4,
        [e0, e1, vir, own, near], [dense, *doubles, lines], [col, amp, bar, bar])
    density, *firsts, far_amp, traces = call(
        functools.partial(first_kernel, weights), 3,
        [e0, e1, e2, e3, vir, far, *blocks, first, first_core, density, traces],
        [dense, *doubles, (square, F32), lines], [col, amp, bar, bar])
    *pair, amps = call(
        middle_kernel, 1,
        [e0, e2, vir, far, *blocks, *firsts, far_amp, second], [*doubles, ((2, *square), F32)], [col])
    *rest, bars_h, bars_l, crosses, traces = call(
        functools.partial(amps_kernel, weights), 4,
        [e0, e1, e2, e3, vir, far, *blocks, *pair, amps, *firsts, second_core, traces],
        [*doubles, ((3, *square), BF16), ((3, *square), BF16), ((2, *square), F32), lines],
        [pltpu.VMEM((2, *square), F32), col])

    def add(before, *terms, span=slice(None)):
        slots = tuple((bar_slot, block_slot, span) for bar_slot, _, block_slot, _ in terms)
        arrays = [array for _, some_bars, _, some_blocks in terms for array in (*some_bars, *some_blocks)]
        return call(
            functools.partial(add_kernel, slots), len(terms), [before, *arrays], [dense], [])[0]

    def part(start, factor, two_away, three_away, traces):
        out = lines if factor is None else ((1, 128), F32)
        *parts, bar_h, bar_l, traces = call(
            functools.partial(part_kernel, weights, start, factor), 1,
            [e0, e2, e3, vir, far, *blocks, two_away, three_away, crosses, traces],
            [((2 * half, aux), BF16)] * 2 + [((rows, 2 * half), BF16)] * 2 + [out], [col, sums])
        return parts, (bar_h, bar_l), traces

    all_bars = (bars_h, bars_l)
    density = add(density, (0, all_bars, 0, pair), (1, all_bars, 0, rest))
    part_0, part_bars_0, traces = part(0, None, low_part, low_core, traces)
    density = add(density, (2, all_bars, 1, rest))
    density = add(density, (None, part_bars_0, None, part_0))
    scale = 1.0 / (rows * lax.axis_size("vir"))
    part_1, part_bars_1, traces = part(half, scale, high_part, high_core, traces)
    density = add(density, (None, part_bars_1, None, part_1), span=slice(0, half))
    density = add(density, (None, part_bars_1, None, part_1), span=slice(half, 2 * half))
    return density[None], traces


def contract(pattern, former, latter):
    return jnp.einsum(
        pattern, former, latter, precision=lax.Precision.HIGH, preferred_element_type=F32
    )


def gathered_ring(factor, occ_energy, vir_energy):
    own = factor[0]
    occs = lax.axis_size("occ")
    far_vir = permuted(vir_energy, lambda i, v: (i, v ^ 1))
    own_far = permuted(own, lambda i, v: (i, v ^ 1))
    sums_near = vir_energy[:, None] + vir_energy[None, :]
    sums_far = vir_energy[:, None] + far_vir[None, :]
    density, trace_of = 0.0, {}
    for d in range(occs):
        if weight(d, occs) == 0:
            continue
        near = permuted(own, lambda i, v, d=d: (i - d, v))
        far = permuted(near, lambda i, v: (i, v ^ 1))
        pair = occ_energy[0] + permuted(occ_energy, lambda i, v, d=d: (i - d, v))[0]
        amp_near = contract("ap,bp->ab", own, near) / (pair - sums_near)
        amp_far = contract("ap,bp->ab", own, far) / (pair - sums_far)
        cross = contract("ap,bp->ab", near, own_far) / (pair - sums_far)
        bar_near = 2.0 * amp_near - amp_near.T
        bar_far = 2.0 * amp_far - cross
        density = density + weight(d, occs) * (
            contract("ab,bp->ap", bar_near, near) + contract("ab,bp->ap", bar_far, far)
        )
        trace_of[d] = jnp.sum(amp_near * bar_near) + jnp.sum(amp_far * bar_far)
    return density[None], jnp.stack([trace_of[k % occs] for k in range(STEPS)])


def local(factor, occ_energy, vir_energy):
    gathered = gathered_plane if lax.axis_size("occ") == 4 else gathered_ring
    density, traces = gathered(factor, occ_energy, vir_energy)
    virs = lax.axis_size("vir")
    nvir = factor.shape[1] * virs
    if gathered is gathered_ring:
        return density, lax.psum(traces[None] / nvir, "vir")
    apart = 1
    while apart < virs:
        traces = traces + permuted(traces, lambda i, v: (i, v ^ apart))
        apart *= 2
    return density, traces[:, :STEPS]


def solution(mesh):
    placed = (P("occ", "vir", None), P("occ"), P("vir"))
    return jax.shard_map(
        local,
        mesh=mesh,
        in_specs=placed,
        out_specs=(P("occ", "vir", None), P("occ", None)),
        check_vma=False,
    )
```

```python
import functools

import jax
import jax.numpy as jnp
from jax import lax
from jax.experimental import pallas as pl
from jax.experimental.pallas import tpu as pltpu
from jax.sharding import PartitionSpec as P


STEPS = 3
AXES = ("occ", "vir")
F32, BF16 = jnp.float32, jnp.bfloat16
VMEM_LIMIT = 12 * 2**20


def permuted(value, move):
    occs, virs = lax.axis_size("occ"), lax.axis_size("vir")
    route = []
    for i in range(occs):
        for v in range(virs):
            source = move(i, v)
            route.append((source[0] % occs * virs + source[1], i * virs + v))
    return lax.ppermute(value, AXES, route)


def weight(offset, occs):
    return sum(offset == k % occs for k in range(STEPS)) + sum(
        offset == -k % occs for k in range(STEPS)
    )


def split(value):
    high = value.astype(BF16)
    return high, (value - high.astype(F32)).astype(BF16)


def dot(former, latter, transposed):
    contracted = ((1,), (1 if transposed else 0,))
    return lax.dot_general(
        former, latter, (contracted, ((), ())), preferred_element_type=F32
    )


def product(former, latter, transposed):
    (fh, fl), (lh, ll) = former, latter
    return dot(fh, lh, transposed) + dot(fh, ll, transposed) + dot(fl, lh, transposed)


def column(row):
    return jnp.transpose(jnp.broadcast_to(row, (8, row.shape[1])))[:, :1]


def lanes(value):
    return jnp.sum(value, axis=0, keepdims=True)


def is_odd():
    return lax.rem(lax.axis_index("occ"), 2)


def each(rows, body, count=2):
    if count == 1:
        body(slice(None))
        return
    size = rows // count

    def step(m, carry):
        body(pl.ds(pl.multiple_of(m * size, size), size))
        return carry

    lax.fori_loop(0, count, step, 0)


def put_split(high, low, rows):
    def step(m):
        high[m], low[m] = split(rows[m])

    each(rows.shape[0], step, 4)


def start_kernel(weights, e0, e1, vir, own, near, total, blocks_h, blocks_l, traces,
                 col, amp, bar_h, bar_l):
    n = own.shape[0]
    put_split(blocks_h.at[0], blocks_l.at[0], own)
    put_split(blocks_h.at[1], blocks_l.at[1], near)
    total[...] = jnp.zeros(total.shape, F32)
    traces[...] = jnp.zeros(traces.shape, F32)

    def block(k, carry):
        pair = e0[0] + jnp.where(k == 0, e0[0], e1[0])
        scale = jnp.where(k == 0, float(weights[0]), float(weights[1]))
        col[...] = pair - column(vir[...])

        def amps(m):
            amp[m] = product((blocks_h[0, m], blocks_l[0, m]), (blocks_h[k], blocks_l[k]), True) / (
                col[m] - vir[...])

        each(n, amps)
        bar = 2.0 * amp[...] - amp[...].T
        traces[pl.ds(k, 1)] = lanes(amp[...] * bar)
        bar_h[...], bar_l[...] = split(scale * bar)

        def totals(m):
            total[m] += product((bar_h[m], bar_l[m]), (blocks_h[k], blocks_l[k]), False)

        each(n, totals)
        return carry

    lax.fori_loop(0, 2, block, 0)


def first_kernel(weights, e0, e1, e2, e3, vir, far, blocks_h, blocks_l, first, first_core, before,
                 traces_in, total, firsts_h, firsts_l, far_amp, traces, col, amp, bar_h, bar_l):
    n = first.shape[0]
    odd = is_odd()
    put_split(firsts_h.at[0], firsts_l.at[0], first)
    put_split(firsts_h.at[1], firsts_l.at[1], first_core)
    pair = e0[0] + jnp.where(odd == 0, e2[0], e3[0])
    pair_far = e0[0] + jnp.where(odd == 0, e1[0], e0[0])
    scale = jnp.where(odd == 0, float(weights[2]), float(weights[1]))
    col[...] = column(vir[...])

    def amps(m):
        left = (blocks_h[0, m], blocks_l[0, m])
        amp[m] = product(left, (firsts_h[odd], firsts_l[odd]), True) / (pair - col[m] - vir[...])
        far_amp[m] = product(left, (firsts_h[1 - odd], firsts_l[1 - odd]), True) / (
            pair_far - col[m] - far[...])

    each(n, amps)
    bar = 2.0 * amp[...] - amp[...].T
    traces[...] = traces_in[...]
    traces[pl.ds(2 + odd, 1)] = lanes(amp[...] * bar)
    bar_h[...], bar_l[...] = split(scale * bar)

    def totals(m):
        total[m] = before[m] + product((bar_h[m], bar_l[m]), (firsts_h[odd], firsts_l[odd]), False)

    each(n, totals)


def middle_kernel(e0, e2, vir, far, blocks_h, blocks_l, firsts_h, firsts_l, far_amp, second,
                  pair_h, pair_l, amps, col):
    n = second.shape[0]
    odd = is_odd()
    put_split(pair_h.at[odd], pair_l.at[odd], second)
    pair_h[1 - odd], pair_l[1 - odd] = firsts_h[1 - odd], firsts_l[1 - odd]
    amps[1 - odd] = far_amp[...]
    col[...] = column(vir[...])
    row = jnp.where(odd == 0, far[...], vir[...])
    pair = e0[0] + jnp.where(odd == 0, e0[0], e2[0])

    def step(m):
        amps[odd, m] = product(
            (blocks_h[0, m], blocks_l[0, m]), (pair_h[odd], pair_l[odd]), True) / (pair - col[m] - row)

    each(n, step, 1)


def amps_kernel(weights, e0, e1, e2, e3, vir, far, blocks_h, blocks_l, pair_h, pair_l, amps,
                firsts_h, firsts_l, second_core, traces_in,
                rest_h, rest_l, bars_h, bars_l, crosses, traces, rest_amp, col):
    n = second_core.shape[0]
    odd = is_odd()
    put_split(rest_h.at[1 - odd], rest_l.at[1 - odd], second_core)
    rest_h[odd], rest_l[odd] = pair_h[1], pair_l[1]
    rest_amp[odd] = amps[1]
    col[...] = column(vir[...])
    row = jnp.where(odd == 0, vir[...], far[...])
    pair = e0[0] + jnp.where(odd == 0, e3[0], e1[0])
    pair_first = e0[0] + jnp.where(odd == 0, e2[0], e3[0])
    pair_second = e0[0] + jnp.where(odd == 0, e3[0], e2[0])
    traces[...] = traces_in[...]

    def step(m):
        other = (pair_h[0], pair_l[0])
        sums = col[m] + far[...]
        rest_amp[1 - odd, m] = product(
            (blocks_h[0, m], blocks_l[0, m]), (rest_h[1 - odd], rest_l[1 - odd]), True) / (
                pair - col[m] - row)
        own_amp = amps[0, m]
        bars_h[0, m], bars_l[0, m] = split(float(weights[0]) * own_amp)
        cross = product((blocks_h[1, m], blocks_l[1, m]), other, True) / (e0[0] + e1[0] - sums)
        near_amp = rest_amp[0, m]
        bar = 2.0 * near_amp - cross
        traces[0:1] += lanes(own_amp * own_amp)
        traces[1:2] += lanes(near_amp * bar)
        bars_h[1, m], bars_l[1, m] = split(float(weights[1]) * bar)
        crosses[1 - odd, m] = product((rest_h[1, m], rest_l[1, m]), other, True) / (pair_second - sums)
        crosses[odd, m] = product((firsts_h[odd, m], firsts_l[odd, m]), other, True) / (pair_first - sums)

    each(n, step, 1)
    amp = rest_amp[1]
    bar = 2.0 * amp - amp.T
    traces[pl.ds(3 - odd, 1)] = lanes(amp * bar)
    scale = jnp.where(odd == 0, float(weights[1]), float(weights[2]))
    bars_h[2], bars_l[2] = split(scale * bar)


def add_kernel(terms, before, *refs):
    total = refs[-1]

    def step(m):
        value = before[m]
        for k, (bar, block, span) in enumerate(terms):
            bar_h, bar_l, block_h, block_l = refs[4 * k : 4 * k + 4]
            left = tuple(ref[m, span] if bar is None else ref[bar, m, span] for ref in (bar_h, bar_l))
            right = tuple(ref[span] if block is None else ref[block, span] for ref in (block_h, block_l))
            value += product(left, right, False)
        total[m] = value

    each(before.shape[0], step, 1)


def part_kernel(weights, start, factor, e0, e2, e3, vir, far, blocks_h, blocks_l, two_away, three_away,
                crosses, traces_in, rows_h, rows_l, bar_h, bar_l, traces, col, sums):
    size = two_away.shape[0]
    put_split(rows_h.at[:size], rows_l.at[:size], two_away)
    put_split(rows_h.at[size:], rows_l.at[size:], three_away)
    part = slice(start, start + size)
    col[...] = column(vir[...])
    row = jnp.concatenate([e0[0] + e2[0] - far[:, part], e0[0] + e3[0] - far[:, part]], axis=1)
    lane = lax.broadcasted_iota(jnp.int32, (1, 2 * size), 1)
    scale = jnp.where(lane < size, float(weights[2]), float(weights[1]))
    sums[...] = jnp.zeros(sums.shape, F32)

    def step(m):
        amp = product((blocks_h[0, m], blocks_l[0, m]), (rows_h[...], rows_l[...]), True) / (row - col[m])
        bar = 2.0 * amp - jnp.concatenate([crosses[0, m, part], crosses[1, m, part]], axis=1)
        sums[...] += lanes(amp * bar)
        bar_h[m], bar_l[m] = split(scale * bar)

    each(col.shape[0], step, 1)
    two, three = sums[:, :size], sums[:, size:]
    if factor is None:
        traces[...] = traces_in[...]
        traces[2:3, :size] += two
        traces[3:4, :size] += three
        return
    odd = is_odd()
    whole = [jnp.sum(traces_in[k : k + 1], axis=1, keepdims=True) for k in range(4)]
    whole[2] += jnp.sum(two, axis=1, keepdims=True)
    whole[3] += jnp.sum(three, axis=1, keepdims=True)
    lane = lax.broadcasted_iota(jnp.int32, (1, 128), 1)
    by_offset = [whole[0], jnp.where(odd == 1, whole[1], whole[3]), whole[2]]
    traces[...] = sum(jnp.where(lane == k, by_offset[k], 0.0) for k in range(3)) * factor


VMEM = pl.BlockSpec(memory_space=pltpu.VMEM)
SMEM = pl.BlockSpec(memory_space=pltpu.SMEM)


def call(kernel, units, inputs, outputs, scratch):
    rows = outputs[0][0][-2]
    return pl.pallas_call(
        kernel,
        in_specs=[SMEM if value.size == 1 else VMEM for value in inputs],
        out_specs=tuple(VMEM for _ in outputs),
        out_shape=tuple(jax.ShapeDtypeStruct(*o) for o in outputs),
        scratch_shapes=scratch,
        compiler_params=pltpu.CompilerParams(vmem_limit_bytes=VMEM_LIMIT),
        cost_estimate=pl.CostEstimate(
            flops=units * 6 * rows * rows * 1280, bytes_accessed=8 << 20, transcendentals=0
        ),
    )(*inputs)


def gathered_plane(factor, occ_energy, vir_energy):
    own = factor[0]
    rows, aux = own.shape
    half = rows // 2
    occs = lax.axis_size("occ")

    def core(value):
        return permuted(value, lambda i, v: (i ^ 1, v))

    def mixed(value, parity):
        return permuted(value, lambda i, v: (i ^ 2, v) if i % 2 == parity else (i, v ^ 1))

    far_vir = permuted(vir_energy, lambda i, v: (i, v ^ 1))
    e0 = occ_energy
    e1, e2, e3 = (permuted(e0, lambda i, v, m=m: (i ^ m, v)) for m in (1, 2, 3))
    near = core(own)
    first = mixed(own, 0)
    second = mixed(own, 1)
    first_core = core(first)
    low_first, high_first = first[:half], first[half:]
    low_part = mixed(low_first, 1)
    high_part = mixed(high_first, 1)
    second_core = core(second)
    low_core, high_core = core(low_part), core(high_part)

    weights = [weight(d, occs) for d in range(3)]
    vir, far = vir_energy[None, :], far_vir[None, :]

    block, square = (rows, aux), (rows, rows)
    dense = (block, F32)
    doubles = [((2, *block), BF16)] * 2
    lines = ((8, rows), F32)
    bar = pltpu.VMEM(square, BF16)
    col = pltpu.VMEM((rows, 1), F32)
    amp = pltpu.VMEM(square, F32)
    sums = pltpu.VMEM((1, 2 * half), F32)

    density, *blocks, traces = call(
        functools.partial(start_kernel, weights), 4,
        [e0, e1, vir, own, near], [dense, *doubles, lines], [col, amp, bar, bar])
    density, *firsts, far_amp, traces = call(
        functools.partial(first_kernel, weights), 3,
        [e0, e1, e2, e3, vir, far, *blocks, first, first_core, density, traces],
        [dense, *doubles, (square, F32), lines], [col, amp, bar, bar])
    *pair, amps = call(
        middle_kernel, 1,
        [e0, e2, vir, far, *blocks, *firsts, far_amp, second], [*doubles, ((2, *square), F32)], [col])
    *rest, bars_h, bars_l, crosses, traces = call(
        functools.partial(amps_kernel, weights), 4,
        [e0, e1, e2, e3, vir, far, *blocks, *pair, amps, *firsts, second_core, traces],
        [*doubles, ((3, *square), BF16), ((3, *square), BF16), ((2, *square), F32), lines],
        [pltpu.VMEM((2, *square), F32), col])

    def add(before, *terms, span=slice(None)):
        slots = tuple((bar_slot, block_slot, span) for bar_slot, _, block_slot, _ in terms)
        arrays = [array for _, some_bars, _, some_blocks in terms for array in (*some_bars, *some_blocks)]
        return call(
            functools.partial(add_kernel, slots), len(terms), [before, *arrays], [dense], [])[0]

    def part(start, factor, two_away, three_away, traces):
        out = lines if factor is None else ((1, 128), F32)
        *parts, bar_h, bar_l, traces = call(
            functools.partial(part_kernel, weights, start, factor), 1,
            [e0, e2, e3, vir, far, *blocks, two_away, three_away, crosses, traces],
            [((2 * half, aux), BF16)] * 2 + [((rows, 2 * half), BF16)] * 2 + [out], [col, sums])
        return parts, (bar_h, bar_l), traces

    all_bars = (bars_h, bars_l)
    density = add(density, (0, all_bars, 0, pair), (1, all_bars, 0, rest))
    part_0, part_bars_0, traces = part(0, None, low_part, low_core, traces)
    density = add(density, (2, all_bars, 1, rest))
    density = add(density, (None, part_bars_0, None, part_0))
    scale = 1.0 / (rows * lax.axis_size("vir"))
    part_1, part_bars_1, traces = part(half, scale, high_part, high_core, traces)
    density = add(density, (None, part_bars_1, None, part_1), span=slice(0, half))
    density = add(density, (None, part_bars_1, None, part_1), span=slice(half, 2 * half))
    return density[None], traces


def contract(pattern, former, latter):
    return jnp.einsum(
        pattern, former, latter, precision=lax.Precision.HIGH, preferred_element_type=F32
    )


def gathered_ring(factor, occ_energy, vir_energy):
    own = factor[0]
    occs = lax.axis_size("occ")
    far_vir = permuted(vir_energy, lambda i, v: (i, v ^ 1))
    own_far = permuted(own, lambda i, v: (i, v ^ 1))
    sums_near = vir_energy[:, None] + vir_energy[None, :]
    sums_far = vir_energy[:, None] + far_vir[None, :]
    density, trace_of = 0.0, {}
    for d in range(occs):
        if weight(d, occs) == 0:
            continue
        near = permuted(own, lambda i, v, d=d: (i - d, v))
        far = permuted(near, lambda i, v: (i, v ^ 1))
        pair = occ_energy[0] + permuted(occ_energy, lambda i, v, d=d: (i - d, v))[0]
        amp_near = contract("ap,bp->ab", own, near) / (pair - sums_near)
        amp_far = contract("ap,bp->ab", own, far) / (pair - sums_far)
        cross = contract("ap,bp->ab", near, own_far) / (pair - sums_far)
        bar_near = 2.0 * amp_near - amp_near.T
        bar_far = 2.0 * amp_far - cross
        density = density + weight(d, occs) * (
            contract("ab,bp->ap", bar_near, near) + contract("ab,bp->ap", bar_far, far)
        )
        trace_of[d] = jnp.sum(amp_near * bar_near) + jnp.sum(amp_far * bar_far)
    return density[None], jnp.stack([trace_of[k % occs] for k in range(STEPS)])


def local(factor, occ_energy, vir_energy):
    gathered = gathered_plane if lax.axis_size("occ") == 4 else gathered_ring
    density, traces = gathered(factor, occ_energy, vir_energy)
    virs = lax.axis_size("vir")
    nvir = factor.shape[1] * virs
    if gathered is gathered_ring:
        return density, lax.psum(traces[None] / nvir, "vir")
    apart = 1
    while apart < virs:
        traces = traces + permuted(traces, lambda i, v: (i, v ^ apart))
        apart *= 2
    return density, traces[:, :STEPS]


def solution(mesh):
    placed = (P("occ", "vir", None), P("occ"), P("vir"))
    return jax.shard_map(
        local,
        mesh=mesh,
        in_specs=placed,
        out_specs=(P("occ", "vir", None), P("occ", None)),
        check_vma=False,
    )
```

```python
import functools

import jax
import jax.numpy as jnp
from jax import lax
from jax.experimental import pallas as pl
from jax.experimental.pallas import tpu as pltpu
from jax.sharding import PartitionSpec as P


STEPS = 3
AXES = ("occ", "vir")
F32, BF16 = jnp.float32, jnp.bfloat16
VMEM_LIMIT = 12 * 2**20


def permuted(value, move):
    occs, virs = lax.axis_size("occ"), lax.axis_size("vir")
    route = []
    for i in range(occs):
        for v in range(virs):
            source = move(i, v)
            route.append((source[0] % occs * virs + source[1], i * virs + v))
    return lax.ppermute(value, AXES, route)


def weight(offset, occs):
    return sum(offset == k % occs for k in range(STEPS)) + sum(
        offset == -k % occs for k in range(STEPS)
    )


def split(value):
    high = value.astype(BF16)
    return high, (value - high.astype(F32)).astype(BF16)


def dot(former, latter, transposed):
    contracted = ((1,), (1 if transposed else 0,))
    return lax.dot_general(
        former, latter, (contracted, ((), ())), preferred_element_type=F32
    )


def product(former, latter, transposed):
    (fh, fl), (lh, ll) = former, latter
    return dot(fh, lh, transposed) + dot(fh, ll, transposed) + dot(fl, lh, transposed)


def column(row):
    return jnp.transpose(jnp.broadcast_to(row, (8, row.shape[1])))[:, :1]


def lanes(value):
    return jnp.sum(value, axis=0, keepdims=True)


def is_odd():
    return lax.rem(lax.axis_index("occ"), 2)


def each(rows, body, count=2):
    if count == 1:
        body(slice(None))
        return
    size = rows // count

    def step(m, carry):
        body(pl.ds(pl.multiple_of(m * size, size), size))
        return carry

    lax.fori_loop(0, count, step, 0)


def put_split(high, low, rows):
    def step(m):
        high[m], low[m] = split(rows[m])

    each(rows.shape[0], step, 4)


def start_kernel(weights, e0, e1, vir, own, near, total, blocks_h, blocks_l, traces, col,
                 amp, bar_h, bar_l):
    n = own.shape[0]
    put_split(blocks_h.at[0], blocks_l.at[0], own)
    put_split(blocks_h.at[1], blocks_l.at[1], near)
    total[...] = jnp.zeros(total.shape, F32)
    traces[...] = jnp.zeros(traces.shape, F32)
    col[...] = column(vir[...])

    def block(k, carry):
        pair = e0[0] + jnp.where(k == 0, e0[0], e1[0])
        scale = jnp.where(k == 0, float(weights[0]), float(weights[1]))
        row = pair - vir[...]

        def amps(m):
            amp[m] = product((blocks_h[0, m], blocks_l[0, m]), (blocks_h[k], blocks_l[k]), True) / (
                row - col[m])

        each(n, amps)
        bar = 2.0 * amp[...] - amp[...].T
        traces[pl.ds(k, 1)] = lanes(amp[...] * bar)
        bar_h[...], bar_l[...] = split(scale * bar)

        def totals(m):
            total[m] += product((bar_h[m], bar_l[m]), (blocks_h[k], blocks_l[k]), False)

        each(n, totals)
        return carry

    lax.fori_loop(0, 2, block, 0)


def first_kernel(weights, e0, e1, e2, e3, vir, far, blocks_h, blocks_l, first, first_core, before,
                 traces_in, col, total, firsts_h, firsts_l, far_amp, traces, rows, amp, bar_h, bar_l):
    n = first.shape[0]
    odd = is_odd()
    put_split(firsts_h.at[0], firsts_l.at[0], first)
    put_split(firsts_h.at[1], firsts_l.at[1], first_core)
    scale = jnp.where(odd == 0, float(weights[2]), float(weights[1]))
    for k, other in enumerate((e0, e1, e2, e3)):
        rows[k : k + 1] = e0[0] + other[0] - far[...]
        rows[k + 4 : k + 5] = e0[0] + other[0] - vir[...]
    row, row_far = rows[pl.ds(6 + odd, 1)], rows[pl.ds(1 - odd, 1)]

    def amps(m):
        left = (blocks_h[0, m], blocks_l[0, m])
        amp[m] = product(left, (firsts_h[odd], firsts_l[odd]), True) / (row - col[m])
        far_amp[m] = product(left, (firsts_h[1 - odd], firsts_l[1 - odd]), True) / (row_far - col[m])

    each(n, amps)
    bar = 2.0 * amp[...] - amp[...].T
    traces[...] = traces_in[...]
    traces[pl.ds(2 + odd, 1)] = lanes(amp[...] * bar)
    bar_h[...], bar_l[...] = split(scale * bar)

    def totals(m):
        total[m] = before[m] + product((bar_h[m], bar_l[m]), (firsts_h[odd], firsts_l[odd]), False)

    each(n, totals)


def middle_kernel(rows, col, blocks_h, blocks_l, firsts_h, firsts_l, far_amp, second,
                  pair_h, pair_l, amps):
    n = second.shape[0]
    odd = is_odd()
    put_split(pair_h.at[odd], pair_l.at[odd], second)
    pair_h[1 - odd], pair_l[1 - odd] = firsts_h[1 - odd], firsts_l[1 - odd]
    amps[1 - odd] = far_amp[...]
    row = rows[pl.ds(6 * odd, 1)]

    def step(m):
        amps[odd, m] = product(
            (blocks_h[0, m], blocks_l[0, m]), (pair_h[odd], pair_l[odd]), True) / (row - col[m])

    each(n, step, 1)


def amps_kernel(weights, rows, col, blocks_h, blocks_l, pair_h, pair_l, amps,
                firsts_h, firsts_l, second_core, traces_in,
                rest_h, rest_l, bars_h, bars_l, crosses, traces, rest_amp):
    n = second_core.shape[0]
    odd = is_odd()
    put_split(rest_h.at[1 - odd], rest_l.at[1 - odd], second_core)
    rest_h[odd], rest_l[odd] = pair_h[1], pair_l[1]
    rest_amp[odd] = amps[1]
    row = rows[pl.ds(7 - 6 * odd, 1)]
    row_first, row_second = rows[pl.ds(2 + odd, 1)], rows[pl.ds(3 - odd, 1)]
    traces[...] = traces_in[...]

    def step(m):
        other = (pair_h[0], pair_l[0])
        rest_amp[1 - odd, m] = product(
            (blocks_h[0, m], blocks_l[0, m]), (rest_h[1 - odd], rest_l[1 - odd]), True) / (row - col[m])
        own_amp = amps[0, m]
        bars_h[0, m], bars_l[0, m] = split(float(weights[0]) * own_amp)
        cross = product((blocks_h[1, m], blocks_l[1, m]), other, True) / (rows[1:2] - col[m])
        near_amp = rest_amp[0, m]
        bar = 2.0 * near_amp - cross
        traces[0:1] += lanes(own_amp * own_amp)
        traces[1:2] += lanes(near_amp * bar)
        bars_h[1, m], bars_l[1, m] = split(float(weights[1]) * bar)
        crosses[1 - odd, m] = product((rest_h[1, m], rest_l[1, m]), other, True) / (row_second - col[m])
        crosses[odd, m] = product((firsts_h[odd, m], firsts_l[odd, m]), other, True) / (row_first - col[m])

    each(n, step, 1)
    amp = rest_amp[1]
    bar = 2.0 * amp - amp.T
    traces[pl.ds(3 - odd, 1)] = lanes(amp * bar)
    scale = jnp.where(odd == 0, float(weights[1]), float(weights[2]))
    bars_h[2], bars_l[2] = split(scale * bar)


def add_kernel(terms, before, *refs):
    total = refs[-1]

    def step(m):
        value = before[m]
        for k, (bar, block, span) in enumerate(terms):
            bar_h, bar_l, block_h, block_l = refs[4 * k : 4 * k + 4]
            left = tuple(ref[m, span] if bar is None else ref[bar, m, span] for ref in (bar_h, bar_l))
            right = tuple(ref[span] if block is None else ref[block, span] for ref in (block_h, block_l))
            value += product(left, right, False)
        total[m] = value

    each(before.shape[0], step, 1)


def part_kernel(weights, start, factor, rows, col, blocks_h, blocks_l, two_away, three_away,
                crosses, traces_in, rows_h, rows_l, bar_h, bar_l, traces, sums):
    size = two_away.shape[0]
    put_split(rows_h.at[:size], rows_l.at[:size], two_away)
    put_split(rows_h.at[size:], rows_l.at[size:], three_away)
    part = slice(start, start + size)
    row = jnp.concatenate([rows[2:3, part], rows[3:4, part]], axis=1)
    lane = lax.broadcasted_iota(jnp.int32, (1, 2 * size), 1)
    scale = jnp.where(lane < size, float(weights[2]), float(weights[1]))
    sums[...] = jnp.zeros(sums.shape, F32)

    def step(m):
        amp = product((blocks_h[0, m], blocks_l[0, m]), (rows_h[...], rows_l[...]), True) / (row - col[m])
        bar = 2.0 * amp - jnp.concatenate([crosses[0, m, part], crosses[1, m, part]], axis=1)
        sums[...] += lanes(amp * bar)
        bar_h[m], bar_l[m] = split(scale * bar)

    each(col.shape[0], step, 1)
    two, three = sums[:, :size], sums[:, size:]
    if factor is None:
        traces[...] = traces_in[...]
        traces[2:3, :size] += two
        traces[3:4, :size] += three
        return
    odd = is_odd()
    whole = [jnp.sum(traces_in[k : k + 1], axis=1, keepdims=True) for k in range(4)]
    whole[2] += jnp.sum(two, axis=1, keepdims=True)
    whole[3] += jnp.sum(three, axis=1, keepdims=True)
    lane = lax.broadcasted_iota(jnp.int32, (1, 128), 1)
    by_offset = [whole[0], jnp.where(odd == 1, whole[1], whole[3]), whole[2]]
    traces[...] = sum(jnp.where(lane == k, by_offset[k], 0.0) for k in range(3)) * factor


VMEM = pl.BlockSpec(memory_space=pltpu.VMEM)
SMEM = pl.BlockSpec(memory_space=pltpu.SMEM)


def call(kernel, units, inputs, outputs, scratch):
    rows = outputs[0][0][-2]
    return pl.pallas_call(
        kernel,
        in_specs=[SMEM if value.size == 1 else VMEM for value in inputs],
        out_specs=tuple(VMEM for _ in outputs),
        out_shape=tuple(jax.ShapeDtypeStruct(*o) for o in outputs),
        scratch_shapes=scratch,
        compiler_params=pltpu.CompilerParams(vmem_limit_bytes=VMEM_LIMIT),
        cost_estimate=pl.CostEstimate(
            flops=units * 6 * rows * rows * 1280, bytes_accessed=8 << 20, transcendentals=0
        ),
    )(*inputs)


def gathered_plane(factor, occ_energy, vir_energy):
    own = factor[0]
    rows, aux = own.shape
    half = rows // 2
    occs = lax.axis_size("occ")

    def core(value):
        return permuted(value, lambda i, v: (i ^ 1, v))

    def mixed(value, parity):
        return permuted(value, lambda i, v: (i ^ 2, v) if i % 2 == parity else (i, v ^ 1))

    far_vir = permuted(vir_energy, lambda i, v: (i, v ^ 1))
    e0 = occ_energy
    e1, e2, e3 = (permuted(e0, lambda i, v, m=m: (i ^ m, v)) for m in (1, 2, 3))
    near = core(own)
    first = mixed(own, 0)
    second = mixed(own, 1)
    first_core = core(first)
    low_first, high_first = first[:half], first[half:]
    low_part = mixed(low_first, 1)
    high_part = mixed(high_first, 1)
    second_core = core(second)
    low_core, high_core = core(low_part), core(high_part)

    weights = [weight(d, occs) for d in range(3)]
    vir, far = vir_energy[None, :], far_vir[None, :]

    block, square = (rows, aux), (rows, rows)
    dense = (block, F32)
    doubles = [((2, *block), BF16)] * 2
    lines = ((8, rows), F32)
    bar = pltpu.VMEM(square, BF16)
    column_out = ((rows, 1), F32)
    amp = pltpu.VMEM(square, F32)
    sums = pltpu.VMEM((1, 2 * half), F32)

    density, *blocks, traces, col = call(
        functools.partial(start_kernel, weights), 4,
        [e0, e1, vir, own, near], [dense, *doubles, lines, column_out], [amp, bar, bar])
    density, *firsts, far_amp, traces, gap_rows = call(
        functools.partial(first_kernel, weights), 3,
        [e0, e1, e2, e3, vir, far, *blocks, first, first_core, density, traces, col],
        [dense, *doubles, (square, F32), lines, lines], [amp, bar, bar])
    *pair, amps = call(
        middle_kernel, 1,
        [gap_rows, col, *blocks, *firsts, far_amp, second], [*doubles, ((2, *square), F32)], [])
    *rest, bars_h, bars_l, crosses, traces = call(
        functools.partial(amps_kernel, weights), 4,
        [gap_rows, col, *blocks, *pair, amps, *firsts, second_core, traces],
        [*doubles, ((3, *square), BF16), ((3, *square), BF16), ((2, *square), F32), lines],
        [pltpu.VMEM((2, *square), F32)])

    def add(before, *terms, span=slice(None)):
        slots = tuple((bar_slot, block_slot, span) for bar_slot, _, block_slot, _ in terms)
        arrays = [array for _, some_bars, _, some_blocks in terms for array in (*some_bars, *some_blocks)]
        return call(
            functools.partial(add_kernel, slots), len(terms), [before, *arrays], [dense], [])[0]

    def part(start, factor, two_away, three_away, traces):
        out = lines if factor is None else ((1, 128), F32)
        *parts, bar_h, bar_l, traces = call(
            functools.partial(part_kernel, weights, start, factor), 1,
            [gap_rows, col, *blocks, two_away, three_away, crosses, traces],
            [((2 * half, aux), BF16)] * 2 + [((rows, 2 * half), BF16)] * 2 + [out], [sums])
        return parts, (bar_h, bar_l), traces

    all_bars = (bars_h, bars_l)
    density = add(density, (0, all_bars, 0, pair), (1, all_bars, 0, rest))
    part_0, part_bars_0, traces = part(0, None, low_part, low_core, traces)
    density = add(density, (2, all_bars, 1, rest))
    density = add(density, (None, part_bars_0, None, part_0))
    scale = 1.0 / (rows * lax.axis_size("vir"))
    part_1, part_bars_1, traces = part(half, scale, high_part, high_core, traces)
    density = add(density, (None, part_bars_1, None, part_1), span=slice(0, half))
    density = add(density, (None, part_bars_1, None, part_1), span=slice(half, 2 * half))
    return density[None], traces


def contract(pattern, former, latter):
    return jnp.einsum(
        pattern, former, latter, precision=lax.Precision.HIGH, preferred_element_type=F32
    )


def gathered_ring(factor, occ_energy, vir_energy):
    own = factor[0]
    occs = lax.axis_size("occ")
    far_vir = permuted(vir_energy, lambda i, v: (i, v ^ 1))
    own_far = permuted(own, lambda i, v: (i, v ^ 1))
    sums_near = vir_energy[:, None] + vir_energy[None, :]
    sums_far = vir_energy[:, None] + far_vir[None, :]
    density, trace_of = 0.0, {}
    for d in range(occs):
        if weight(d, occs) == 0:
            continue
        near = permuted(own, lambda i, v, d=d: (i - d, v))
        far = permuted(near, lambda i, v: (i, v ^ 1))
        pair = occ_energy[0] + permuted(occ_energy, lambda i, v, d=d: (i - d, v))[0]
        amp_near = contract("ap,bp->ab", own, near) / (pair - sums_near)
        amp_far = contract("ap,bp->ab", own, far) / (pair - sums_far)
        cross = contract("ap,bp->ab", near, own_far) / (pair - sums_far)
        bar_near = 2.0 * amp_near - amp_near.T
        bar_far = 2.0 * amp_far - cross
        density = density + weight(d, occs) * (
            contract("ab,bp->ap", bar_near, near) + contract("ab,bp->ap", bar_far, far)
        )
        trace_of[d] = jnp.sum(amp_near * bar_near) + jnp.sum(amp_far * bar_far)
    return density[None], jnp.stack([trace_of[k % occs] for k in range(STEPS)])


def local(factor, occ_energy, vir_energy):
    gathered = gathered_plane if lax.axis_size("occ") == 4 else gathered_ring
    density, traces = gathered(factor, occ_energy, vir_energy)
    virs = lax.axis_size("vir")
    nvir = factor.shape[1] * virs
    if gathered is gathered_ring:
        return density, lax.psum(traces[None] / nvir, "vir")
    apart = 1
    while apart < virs:
        traces = traces + permuted(traces, lambda i, v: (i, v ^ apart))
        apart *= 2
    return density, traces[:, :STEPS]


def solution(mesh):
    placed = (P("occ", "vir", None), P("occ"), P("vir"))
    return jax.shard_map(
        local,
        mesh=mesh,
        in_specs=placed,
        out_specs=(P("occ", "vir", None), P("occ", None)),
        check_vma=False,
    )
```

```python
import functools

import jax
import jax.numpy as jnp
from jax import lax
from jax.experimental import pallas as pl
from jax.experimental.pallas import tpu as pltpu
from jax.sharding import PartitionSpec as P


STEPS = 3
AXES = ("occ", "vir")
F32, BF16 = jnp.float32, jnp.bfloat16
VMEM_LIMIT = 12 * 2**20


def permuted(value, move):
    occs, virs = lax.axis_size("occ"), lax.axis_size("vir")
    route = []
    for i in range(occs):
        for v in range(virs):
            source = move(i, v)
            route.append((source[0] % occs * virs + source[1], i * virs + v))
    return lax.ppermute(value, AXES, route)


def weight(offset, occs):
    return sum(offset == k % occs for k in range(STEPS)) + sum(
        offset == -k % occs for k in range(STEPS)
    )


def split(value):
    high = value.astype(BF16)
    return high, (value - high.astype(F32)).astype(BF16)


def dot(former, latter, transposed):
    contracted = ((1,), (1 if transposed else 0,))
    return lax.dot_general(
        former, latter, (contracted, ((), ())), preferred_element_type=F32
    )


def product(former, latter, transposed):
    (fh, fl), (lh, ll) = former, latter
    return dot(fh, lh, transposed) + dot(fh, ll, transposed) + dot(fl, lh, transposed)


def column(row):
    return jnp.transpose(jnp.broadcast_to(row, (8, row.shape[1])))[:, :1]


def lanes(value):
    return jnp.sum(value, axis=0, keepdims=True)


def is_odd():
    return lax.rem(lax.axis_index("occ"), 2)


def each(rows, body, count=2):
    if count == 1:
        body(slice(None))
        return
    size = rows // count

    def step(m, carry):
        body(pl.ds(pl.multiple_of(m * size, size), size))
        return carry

    lax.fori_loop(0, count, step, 0)


def put_split(high, low, rows):
    def step(m):
        high[m], low[m] = split(rows[m])

    each(rows.shape[0], step, 4)


def by_offset(sums, factor):
    lane = lax.broadcasted_iota(jnp.int32, (1, 128), 1)
    terms = [sums[0], jnp.where(is_odd() == 1, sums[1], sums[3]), sums[2]]
    return sum(jnp.where(lane == k, term * factor, 0.0) for k, term in enumerate(terms))


def start_kernel(weights, e0, e1, vir, own, near, total, blocks_h, blocks_l, traces, col,
                 amp, bar_h, bar_l):
    n = own.shape[0]
    put_split(blocks_h.at[0], blocks_l.at[0], own)
    put_split(blocks_h.at[1], blocks_l.at[1], near)
    total[...] = jnp.zeros(total.shape, F32)
    traces[...] = jnp.zeros(traces.shape, F32)
    col[...] = column(vir[...])

    def block(k, carry):
        pair = e0[0] + jnp.where(k == 0, e0[0], e1[0])
        scale = jnp.where(k == 0, float(weights[0]), float(weights[1]))
        row = pair - vir[...]

        def amps(m):
            amp[m] = product((blocks_h[0, m], blocks_l[0, m]), (blocks_h[k], blocks_l[k]), True) / (
                row - col[m])

        each(n, amps)
        bar = 2.0 * amp[...] - amp[...].T
        traces[pl.ds(k, 1)] = lanes(amp[...] * bar)
        bar_h[...], bar_l[...] = split(scale * bar)

        def totals(m):
            total[m] += product((bar_h[m], bar_l[m]), (blocks_h[k], blocks_l[k]), False)

        each(n, totals)
        return carry

    lax.fori_loop(0, 2, block, 0)


def first_kernel(weights, e0, e1, e2, e3, vir, far, blocks_h, blocks_l, first, first_core, before,
                 traces_in, col, total, firsts_h, firsts_l, far_amp, traces, rows, amp, bar_h, bar_l):
    n = first.shape[0]
    odd = is_odd()
    put_split(firsts_h.at[0], firsts_l.at[0], first)
    put_split(firsts_h.at[1], firsts_l.at[1], first_core)
    scale = jnp.where(odd == 0, float(weights[2]), float(weights[1]))
    for k, other in enumerate((e0, e1, e2, e3)):
        rows[k : k + 1] = e0[0] + other[0] - far[...]
        rows[k + 4 : k + 5] = e0[0] + other[0] - vir[...]
    row, row_far = rows[pl.ds(6 + odd, 1)], rows[pl.ds(1 - odd, 1)]

    def amps(m):
        left = (blocks_h[0, m], blocks_l[0, m])
        amp[m] = product(left, (firsts_h[odd], firsts_l[odd]), True) / (row - col[m])
        far_amp[m] = product(left, (firsts_h[1 - odd], firsts_l[1 - odd]), True) / (row_far - col[m])

    each(n, amps)
    bar = 2.0 * amp[...] - amp[...].T
    traces[...] = traces_in[...]
    traces[pl.ds(2 + odd, 1)] = lanes(amp[...] * bar)
    bar_h[...], bar_l[...] = split(scale * bar)

    def totals(m):
        total[m] = before[m] + product((bar_h[m], bar_l[m]), (firsts_h[odd], firsts_l[odd]), False)

    each(n, totals)


def middle_kernel(rows, col, blocks_h, blocks_l, firsts_h, firsts_l, far_amp, second,
                  pair_h, pair_l, amps):
    n = second.shape[0]
    odd = is_odd()
    put_split(pair_h.at[odd], pair_l.at[odd], second)
    pair_h[1 - odd], pair_l[1 - odd] = firsts_h[1 - odd], firsts_l[1 - odd]
    amps[1 - odd] = far_amp[...]
    row = rows[pl.ds(6 * odd, 1)]

    def step(m):
        amps[odd, m] = product(
            (blocks_h[0, m], blocks_l[0, m]), (pair_h[odd], pair_l[odd]), True) / (row - col[m])

    each(n, step, 1)


def amps_kernel(weights, factor, rows, col, blocks_h, blocks_l, pair_h, pair_l, amps,
                firsts_h, firsts_l, second_core, traces_in,
                rest_h, rest_l, bars_h, bars_l, crosses, trace, rest_amp, traces):
    n = second_core.shape[0]
    odd = is_odd()
    put_split(rest_h.at[1 - odd], rest_l.at[1 - odd], second_core)
    rest_h[odd], rest_l[odd] = pair_h[1], pair_l[1]
    rest_amp[odd] = amps[1]
    row = rows[pl.ds(7 - 6 * odd, 1)]
    row_first, row_second = rows[pl.ds(2 + odd, 1)], rows[pl.ds(3 - odd, 1)]
    traces[...] = traces_in[...]

    def step(m):
        other = (pair_h[0], pair_l[0])
        rest_amp[1 - odd, m] = product(
            (blocks_h[0, m], blocks_l[0, m]), (rest_h[1 - odd], rest_l[1 - odd]), True) / (row - col[m])
        own_amp = amps[0, m]
        bars_h[0, m], bars_l[0, m] = split(float(weights[0]) * own_amp)
        cross = product((blocks_h[1, m], blocks_l[1, m]), other, True) / (rows[1:2] - col[m])
        near_amp = rest_amp[0, m]
        bar = 2.0 * near_amp - cross
        traces[0:1] += lanes(own_amp * own_amp)
        traces[1:2] += lanes(near_amp * bar)
        bars_h[1, m], bars_l[1, m] = split(float(weights[1]) * bar)
        crosses[1 - odd, m] = product((rest_h[1, m], rest_l[1, m]), other, True) / (row_second - col[m])
        crosses[odd, m] = product((firsts_h[odd, m], firsts_l[odd, m]), other, True) / (row_first - col[m])

    each(n, step, 1)
    amp = rest_amp[1]
    bar = 2.0 * amp - amp.T
    traces[pl.ds(3 - odd, 1)] = lanes(amp * bar)
    scale = jnp.where(odd == 0, float(weights[1]), float(weights[2]))
    bars_h[2], bars_l[2] = split(scale * bar)
    trace[...] = by_offset(
        [jnp.sum(traces[k : k + 1], axis=1, keepdims=True) for k in range(4)], factor)


def add_kernel(terms, before, *refs):
    total = refs[-1]

    def step(m):
        value = before[m]
        for k, (bar, block, span) in enumerate(terms):
            bar_h, bar_l, block_h, block_l = refs[4 * k : 4 * k + 4]
            left = tuple(ref[m, span] if bar is None else ref[bar, m, span] for ref in (bar_h, bar_l))
            right = tuple(ref[span] if block is None else ref[block, span] for ref in (block_h, block_l))
            value += product(left, right, False)
        total[m] = value

    each(before.shape[0], step, 1)


def part_kernel(weights, start, factor, rows, col, blocks_h, blocks_l, two_away, three_away,
                crosses, *refs):
    before, trace_in, trace_far = refs[:3] if factor else (None, None, None)
    rows_h, rows_l, bar_h, bar_l, out = refs[-6:-1] if factor else refs[-5:]
    sums = refs[-1]
    size = two_away.shape[0]
    put_split(rows_h.at[:size], rows_l.at[:size], two_away)
    put_split(rows_h.at[size:], rows_l.at[size:], three_away)
    part = slice(start, start + size)
    row = jnp.concatenate([rows[2:3, part], rows[3:4, part]], axis=1)
    lane = lax.broadcasted_iota(jnp.int32, (1, 2 * size), 1)
    scale = jnp.where(lane < size, float(weights[2]), float(weights[1]))
    sums[...] = before[...] if factor else jnp.zeros(sums.shape, F32)

    def step(m):
        amp = product((blocks_h[0, m], blocks_l[0, m]), (rows_h[...], rows_l[...]), True) / (row - col[m])
        cross = jnp.concatenate([crosses[0, m, part], crosses[1, m, part]], axis=1)
        bar = 2.0 * amp - cross
        sums[...] += lanes(amp * bar + cross * (2.0 * cross - amp))
        bar_h[m], bar_l[m] = split(scale * bar)

    each(col.shape[0], step, 1)
    if not factor:
        return
    two = jnp.sum(sums[:, :size], axis=1, keepdims=True)
    three = jnp.sum(sums[:, size:], axis=1, keepdims=True)
    zero = jnp.zeros_like(two)
    out[...] = trace_in[...] + trace_far[...] + by_offset([zero, zero, two, three], factor)


VMEM = pl.BlockSpec(memory_space=pltpu.VMEM)
SMEM = pl.BlockSpec(memory_space=pltpu.SMEM)


def call(kernel, units, inputs, outputs, scratch):
    rows = outputs[0][0][-2]
    return pl.pallas_call(
        kernel,
        in_specs=[SMEM if value.size == 1 else VMEM for value in inputs],
        out_specs=tuple(VMEM for _ in outputs),
        out_shape=tuple(jax.ShapeDtypeStruct(*o) for o in outputs),
        scratch_shapes=scratch,
        compiler_params=pltpu.CompilerParams(vmem_limit_bytes=VMEM_LIMIT),
        cost_estimate=pl.CostEstimate(
            flops=units * 6 * rows * rows * 1280, bytes_accessed=8 << 20, transcendentals=0
        ),
    )(*inputs)


def gathered_plane(factor, occ_energy, vir_energy):
    own = factor[0]
    rows, aux = own.shape
    half = rows // 2
    occs = lax.axis_size("occ")

    def core(value):
        return permuted(value, lambda i, v: (i ^ 1, v))

    def mixed(value, parity):
        return permuted(value, lambda i, v: (i ^ 2, v) if i % 2 == parity else (i, v ^ 1))

    far_vir = permuted(vir_energy, lambda i, v: (i, v ^ 1))
    e0 = occ_energy
    e1, e2, e3 = (permuted(e0, lambda i, v, m=m: (i ^ m, v)) for m in (1, 2, 3))
    near = core(own)
    first = mixed(own, 0)
    second = mixed(own, 1)
    first_core = core(first)
    low_first, high_first = first[:half], first[half:]
    low_part = mixed(low_first, 1)
    high_part = mixed(high_first, 1)
    second_core = core(second)
    low_core, high_core = core(low_part), core(high_part)

    weights = [weight(d, occs) for d in range(3)]
    vir, far = vir_energy[None, :], far_vir[None, :]

    block, square = (rows, aux), (rows, rows)
    dense = (block, F32)
    doubles = [((2, *block), BF16)] * 2
    lines = ((8, rows), F32)
    bar = pltpu.VMEM(square, BF16)
    column_out = ((rows, 1), F32)
    amp = pltpu.VMEM(square, F32)
    sums = pltpu.VMEM((1, 2 * half), F32)

    density, *blocks, traces, col = call(
        functools.partial(start_kernel, weights), 4,
        [e0, e1, vir, own, near], [dense, *doubles, lines, column_out], [amp, bar, bar])
    density, *firsts, far_amp, traces, gap_rows = call(
        functools.partial(first_kernel, weights), 3,
        [e0, e1, e2, e3, vir, far, *blocks, first, first_core, density, traces, col],
        [dense, *doubles, (square, F32), lines, lines], [amp, bar, bar])
    *pair, amps = call(
        middle_kernel, 1,
        [gap_rows, col, *blocks, *firsts, far_amp, second], [*doubles, ((2, *square), F32)], [])
    scale = 1.0 / (rows * lax.axis_size("vir"))
    *rest, bars_h, bars_l, crosses, trace = call(
        functools.partial(amps_kernel, weights, scale), 4,
        [gap_rows, col, *blocks, *pair, amps, *firsts, second_core, traces],
        [*doubles, ((3, *square), BF16), ((3, *square), BF16), ((2, *square), F32), ((1, 128), F32)],
        [pltpu.VMEM((2, *square), F32), pltpu.VMEM((8, rows), F32)])
    trace_far = permuted(trace, lambda i, v: (i, v ^ 1))

    def add(before, *terms, span=slice(None)):
        slots = tuple((bar_slot, block_slot, span) for bar_slot, _, block_slot, _ in terms)
        arrays = [array for _, some_bars, _, some_blocks in terms for array in (*some_bars, *some_blocks)]
        return call(
            functools.partial(add_kernel, slots), len(terms), [before, *arrays], [dense], [])[0]

    def part(start, factor, two_away, three_away, *more):
        out, scratch = (((1, 128), F32), [sums]) if factor else (((1, 2 * half), F32), [])
        *parts, bar_h, bar_l, out = call(
            functools.partial(part_kernel, weights, start, factor), 1,
            [gap_rows, col, *blocks, two_away, three_away, crosses, *more],
            [((2 * half, aux), BF16)] * 2 + [((rows, 2 * half), BF16)] * 2 + [out], scratch)
        return parts, (bar_h, bar_l), out

    all_bars = (bars_h, bars_l)
    density = add(density, (0, all_bars, 0, pair), (1, all_bars, 0, rest))
    part_0, part_bars_0, part_sums = part(0, None, low_part, low_core)
    density = add(density, (2, all_bars, 1, rest))
    density = add(density, (None, part_bars_0, None, part_0))
    part_1, part_bars_1, trace = part(
        half, scale, high_part, high_core, part_sums, trace, trace_far)
    density = add(density, (None, part_bars_1, None, part_1), span=slice(0, half))
    density = add(density, (None, part_bars_1, None, part_1), span=slice(half, 2 * half))
    return density[None], trace


def contract(pattern, former, latter):
    return jnp.einsum(
        pattern, former, latter, precision=lax.Precision.HIGH, preferred_element_type=F32
    )


def gathered_ring(factor, occ_energy, vir_energy):
    own = factor[0]
    occs = lax.axis_size("occ")
    far_vir = permuted(vir_energy, lambda i, v: (i, v ^ 1))
    own_far = permuted(own, lambda i, v: (i, v ^ 1))
    sums_near = vir_energy[:, None] + vir_energy[None, :]
    sums_far = vir_energy[:, None] + far_vir[None, :]
    density, trace_of = 0.0, {}
    for d in range(occs):
        if weight(d, occs) == 0:
            continue
        near = permuted(own, lambda i, v, d=d: (i - d, v))
        far = permuted(near, lambda i, v: (i, v ^ 1))
        pair = occ_energy[0] + permuted(occ_energy, lambda i, v, d=d: (i - d, v))[0]
        amp_near = contract("ap,bp->ab", own, near) / (pair - sums_near)
        amp_far = contract("ap,bp->ab", own, far) / (pair - sums_far)
        cross = contract("ap,bp->ab", near, own_far) / (pair - sums_far)
        bar_near = 2.0 * amp_near - amp_near.T
        bar_far = 2.0 * amp_far - cross
        density = density + weight(d, occs) * (
            contract("ab,bp->ap", bar_near, near) + contract("ab,bp->ap", bar_far, far)
        )
        trace_of[d] = jnp.sum(amp_near * bar_near) + jnp.sum(amp_far * bar_far)
    return density[None], jnp.stack([trace_of[k % occs] for k in range(STEPS)])


def local(factor, occ_energy, vir_energy):
    gathered = gathered_plane if lax.axis_size("occ") == 4 else gathered_ring
    density, traces = gathered(factor, occ_energy, vir_energy)
    virs = lax.axis_size("vir")
    nvir = factor.shape[1] * virs
    if gathered is gathered_ring:
        return density, lax.psum(traces[None] / nvir, "vir")
    apart = 2
    while apart < virs:
        traces = traces + permuted(traces, lambda i, v: (i, v ^ apart))
        apart *= 2
    return density, traces[:, :STEPS]


def solution(mesh):
    placed = (P("occ", "vir", None), P("occ"), P("vir"))
    return jax.shard_map(
        local,
        mesh=mesh,
        in_specs=placed,
        out_specs=(P("occ", "vir", None), P("occ", None)),
        check_vma=False,
    )
```
